256 devices in a mesh: member: 4 (over x, y), block: 64 (over z, core).
Axes of the slice: x: 2, y: 2, z: 32, core: 2. Of those that a mesh axis runs over, the one named last changes fastest.
The devices are a block of a 4x8x32 slice.
Arguments:
- grid_in: bfloat16 [262144, 128], P(('member', 'block')), parts along dimension 0, may hold values from -6 to 6
- dest_block: int32 [262144, 1], P(('member', 'block')), parts along dimension 0, may hold values from 0 to 63, as said below
- dest_node: int32 [262144], P(('member', 'block')), parts along dimension 0, may hold values from 0 to 255
- neighbour_mask: int32 [65536, 4], P(('member', 'block')), parts along dimension 0, may hold values 0 or 1
- mesh_embed: bfloat16 [65536, 512], P(('member', 'block')), parts along dimension 0, may hold values from -6 to 6
- w_in: bfloat16 [128, 512], replicated, may hold values from -0.5 to 0.5
- in_bias: bfloat16 [512], replicated, may hold values from -3 to 3
- w_grid: bfloat16 [512, 512], replicated, may hold values from -0.25 to 0.25
- w_enc: bfloat16 [512, 512], replicated, may hold values from -0.25 to 0.25
- attn_gain: bfloat16 [2, 512], replicated, may hold values from 0.099609375 to 1.8984375
- w_query: bfloat16 [2, 512, 512], replicated, may hold values from -0.25 to 0.25
- w_key: bfloat16 [2, 512, 512], replicated, may hold values from -0.25 to 0.25
- w_value: bfloat16 [2, 512, 512], replicated, may hold values from -0.25 to 0.25
- w_out: bfloat16 [2, 512, 512], replicated, may hold values from -0.25 to 0.25
- mlp_gain: bfloat16 [2, 512], replicated, may hold values from 0.099609375 to 1.8984375
- w_up: bfloat16 [2, 512, 512], replicated, may hold values from -0.25 to 0.25
- w_down: bfloat16 [2, 512, 512], replicated, may hold values from -0.25 to 0.25
- dec_gain: bfloat16 [512], replicated, may hold values from 0.099609375 to 1.8984375
- w_dec: bfloat16 [512, 512], replicated, may hold values from -0.25 to 0.25
- w_head: bfloat16 [512, 512], replicated, may hold values from -0.25 to 0.25
- w_final: bfloat16 [512, 128], replicated, may hold values from -0.25 to 0.25
Outputs:
- grid_out: bfloat16 [262144, 128], P(('member', 'block')), parts along dimension 0
The draws below stay inside these ranges and needn't reach their ends.
There are 4 independent parts, one for each index of `member`. The reference program is written for one: setup_inputs(seed, part) draws one part's arguments, and reference() takes and returns one part's arrays. A program takes and returns all parts, laid end to end along the dimension named above; an argument that names none is the same for every part. Nothing has to cross between parts.
Inputs may be any that keep to these rules, and one draw needn't show every extreme that they name: `dest_block`: A grid point of block b maps into one of the mesh blocks b-2, b-1, b, b+1, b+2 (modulo 64); within the 1024 rows of one block exactly 512 name one of these five, and the others name fewer.
All inputs are finite; a program needn't handle non-finite values. No bound on the sum of `neighbour_mask` on one device may be relied on, other than what follows from the above.
Results may differ from the reference program's by a relative error of at most 0.014.
Values may be sent and summed in bfloat16 or wider, within the bound.
A program may use at most 64 MiB of HBM per device.

```python
import jax
import jax.numpy as jnp
from jax import lax

D = 512
IN = 128
HEADS = 8
LAYERS = 2
GRID_DEV = 1024
MESH_DEV = 256
GRID = 65536
N_NODES = 16384
N_BLOCK = 64


def draw_dest_block(key, part):
    key_heavy = jax.random.fold_in(key, 11)
    key_other = jax.random.fold_in(key, 12)
    key_order = jax.random.fold_in(key, 13)
    heavy = jax.random.randint(key_heavy, (N_BLOCK, 1), 0, 5)
    others = jax.random.randint(key_other, (N_BLOCK, GRID_DEV), 1, 5)
    ranks = jax.vmap(lambda k: jax.random.permutation(k, GRID_DEV))(jax.random.split(key_order, N_BLOCK))
    picked = jnp.where(ranks < GRID_DEV // 2, heavy, (heavy + others) % 5)
    blocks = jnp.arange(N_BLOCK, dtype=jnp.int32)[:, None]
    dest = (blocks + picked.astype(jnp.int32) - 2) % N_BLOCK
    return dest.reshape(GRID, 1).astype(jnp.int32)


def place_ends(result, own_key, low, high):
    extent = result.shape
    place = [jax.random.randint(jax.random.fold_in(own_key, axis), (), 0, extent[axis]) for axis in range(len(extent))]
    result = result.at[tuple(place)].set(low)
    longest = extent.index(max(extent))
    place[longest] = (place[longest] + 1) % extent[longest]
    return result.at[tuple(place)].set(high)


def block_levels(own_key, extent, cuts, least, high):
    level, own = 1.0, jax.random.fold_in(own_key, 6)
    for position, blocks in cuts:
        heights = jnp.exp(jax.random.uniform(jax.random.fold_in(own, position), (blocks,), jnp.float32, least / len(cuts), high / len(cuts)))
        level = level * jnp.repeat(heights, extent[position] // blocks).reshape([-1 if axis == position else 1 for axis in range(len(extent))])
    return level


def normal_values(key, extent, deviation, most, cuts=(), kind=jnp.bfloat16):
    array = jax.random.normal(key, extent, jnp.float32) * deviation
    if len(cuts) > 0:
        array = block_levels(key, extent, cuts, -0.22, 0.18) * array
    return jnp.clip(array, min=-most, max=most).astype(kind)


def setup_inputs(seed: int = 0, part: int = 0) -> dict:
    seeds = jax.random.split(jax.random.key(seed), 22)
    own_keys = jax.random.split(jax.random.fold_in(seeds[21], part), 22)
    return {
        "grid_in": normal_values(own_keys[0], (GRID, IN), 1.0, 6.0, ((0, 64),)),
        "dest_block": draw_dest_block(jax.random.fold_in(jax.random.fold_in(seeds[21], part), 71), part),
        "dest_node": place_ends(jax.random.randint(own_keys[2], (GRID,), 0, MESH_DEV), jax.random.fold_in(own_keys[2], 1), 0, MESH_DEV - 1).astype(jnp.int32),
        "neighbour_mask": place_ends((jax.random.randint(own_keys[3], (N_NODES, 4), 0, 4) < 3).astype(jnp.int32), jax.random.fold_in(own_keys[3], 1), 0, 1),
        "mesh_embed": normal_values(own_keys[4], (N_NODES, D), 1.0, 6.0, ((0, 64),)),
        "w_in": normal_values(seeds[5], (IN, D), IN ** -0.5, 0.5),
        "in_bias": normal_values(seeds[6], (D,), 0.5, 3.0),
        "w_grid": normal_values(seeds[7], (D, D), D ** -0.5, 0.25),
        "w_enc": normal_values(seeds[8], (D, D), D ** -0.5, 0.25),
        "attn_gain": jnp.clip(1.0 + 0.18 * jax.random.normal(seeds[9], (LAYERS, D), jnp.float32), 0.099609375, 1.8984375).astype(jnp.bfloat16),
        "w_query": normal_values(seeds[10], (LAYERS, D, D), D ** -0.5, 0.25),
        "w_key": normal_values(seeds[11], (LAYERS, D, D), D ** -0.5, 0.25),
        "w_value": normal_values(seeds[12], (LAYERS, D, D), D ** -0.5, 0.25),
        "w_out": normal_values(seeds[13], (LAYERS, D, D), D ** -0.5, 0.25),
        "mlp_gain": jnp.clip(1.0 + 0.18 * jax.random.normal(seeds[14], (LAYERS, D), jnp.float32), 0.099609375, 1.8984375).astype(jnp.bfloat16),
        "w_up": normal_values(seeds[15], (LAYERS, D, D), D ** -0.5, 0.25),
        "w_down": normal_values(seeds[16], (LAYERS, D, D), D ** -0.5, 0.25),
        "dec_gain": jnp.clip(1.0 + 0.18 * jax.random.normal(seeds[17], (D,), jnp.float32), 0.099609375, 1.8984375).astype(jnp.bfloat16),
        "w_dec": normal_values(seeds[18], (D, D), D ** -0.5, 0.25),
        "w_head": normal_values(seeds[19], (D, D), D ** -0.5, 0.25),
        "w_final": normal_values(seeds[20], (D, IN), D ** -0.5, 0.25),
    }


def rms_norm(values, gain):
    return values * lax.rsqrt(lax.optimization_barrier(jnp.mean(values * values, axis=-1, keepdims=True)) + 1e-06) * gain.astype(jnp.float32)

def attend_all(query_rows, key_rows, value_rows, neighbour_mask):
    head_dim = D // HEADS
    query_blocks = query_rows.reshape(N_BLOCK, MESH_DEV, HEADS, head_dim)
    key_blocks = key_rows.reshape(N_BLOCK, MESH_DEV, HEADS, head_dim)
    value_blocks = value_rows.reshape(N_BLOCK, MESH_DEV, HEADS, head_dim)
    mask_blocks = neighbour_mask.reshape(N_BLOCK, MESH_DEV, 4)
    offsets = jnp.arange(-2, 3, dtype=jnp.int32)

    def single(block_index):
        near_blocks = (block_index + offsets) % N_BLOCK
        keys_near = key_blocks[near_blocks].reshape(5 * MESH_DEV, HEADS, head_dim).astype(jnp.float32)
        values_near = value_blocks[near_blocks].reshape(5 * MESH_DEV, HEADS, head_dim).astype(jnp.float32)
        queries = query_blocks[block_index].astype(jnp.float32)
        own_mask = mask_blocks[block_index]
        allowed = jnp.concatenate([own_mask[:, :2], jnp.ones((MESH_DEV, 1), jnp.int32), own_mask[:, 2:]], axis=1) > 0
        scores = jnp.einsum('qhd,khd->hqk', queries, keys_near) * head_dim ** (-0.5)
        scores = jnp.where(allowed[None, :, :, None], scores.reshape(HEADS, MESH_DEV, 5, MESH_DEV), -jnp.inf)
        scores = scores.reshape(HEADS, MESH_DEV, 5 * MESH_DEV)
        largest = lax.optimization_barrier(jnp.max(scores, axis=-1, keepdims=True))
        exponent = jnp.exp(scores - largest)
        softmax_weights = (exponent / lax.optimization_barrier(jnp.sum(exponent, axis=-1, keepdims=True))).astype(jnp.bfloat16)
        attended = jnp.einsum('hqk,khd->qhd', softmax_weights.astype(jnp.float32), values_near)
        return attended.astype(jnp.bfloat16).reshape(MESH_DEV, D)
    return lax.map(single, jnp.arange(N_BLOCK, dtype=jnp.int32)).reshape(N_NODES, D)

def reference(grid_in, dest_block, dest_node, neighbour_mask, mesh_embed, w_in, in_bias, w_grid, w_enc, attn_gain, w_query, w_key, w_value, w_out, mlp_gain, w_up, w_down, dec_gain, w_dec, w_head, w_final):
    grid_hidden = jax.nn.silu(jnp.dot(grid_in, w_in, preferred_element_type=jnp.float32) + in_bias.astype(jnp.float32)).astype(jnp.bfloat16)
    grid_feat = jnp.dot(grid_hidden, w_grid, preferred_element_type=jnp.float32).astype(jnp.bfloat16)
    target = (dest_block[:, 0] * MESH_DEV + dest_node).astype(jnp.int32)
    summed = jnp.zeros((N_NODES, D), jnp.float32).at[target].add(grid_feat.astype(jnp.float32))
    counts = jnp.zeros((N_NODES,), jnp.float32).at[target].add(jnp.ones((GRID,), jnp.float32))
    mean_rows = (summed / jnp.maximum(counts, 1.0)[:, None]).astype(jnp.bfloat16)
    mesh_state = mesh_embed.astype(jnp.float32) + jnp.dot(mean_rows, w_enc, preferred_element_type=jnp.float32)
    for layer_index in range(LAYERS):
        normed = rms_norm(mesh_state, attn_gain[layer_index]).astype(jnp.bfloat16)
        query_rows = jnp.dot(normed, w_query[layer_index], preferred_element_type=jnp.float32).astype(jnp.bfloat16)
        key_rows = jnp.dot(normed, w_key[layer_index], preferred_element_type=jnp.float32).astype(jnp.bfloat16)
        value_rows = jnp.dot(normed, w_value[layer_index], preferred_element_type=jnp.float32).astype(jnp.bfloat16)
        attended = attend_all(query_rows, key_rows, value_rows, neighbour_mask)
        mesh_state = mesh_state + jnp.dot(attended, w_out[layer_index], preferred_element_type=jnp.float32)
        normed_second = rms_norm(mesh_state, mlp_gain[layer_index]).astype(jnp.bfloat16)
        up_hidden = jax.nn.silu(jnp.dot(normed_second, w_up[layer_index], preferred_element_type=jnp.float32)).astype(jnp.bfloat16)
        mesh_state = mesh_state + jnp.dot(up_hidden, w_down[layer_index], preferred_element_type=jnp.float32)
    decoded = rms_norm(mesh_state, dec_gain).astype(jnp.bfloat16)
    gathered = decoded[target]
    grid_mix = (grid_feat.astype(jnp.float32) + jnp.dot(gathered, w_dec, preferred_element_type=jnp.float32)).astype(jnp.bfloat16)
    head_rows = jax.nn.silu(jnp.dot(grid_mix, w_head, preferred_element_type=jnp.float32)).astype(jnp.bfloat16)
    return jnp.dot(head_rows, w_final, preferred_element_type=jnp.float32).astype(jnp.bfloat16)
```

```python
import functools

import jax
import jax.numpy as jnp
from jax import lax
from jax.experimental import pallas as pl
from jax.experimental.pallas import tpu as pltpu
from jax.sharding import PartitionSpec as P

HEADS = 8
LAYERS = 2
PAIRS = HEADS // 2
HALVES = 2
BIG = 1e30
MESH = pl.DeviceIdType.MESH
F32 = jnp.float32
BF16 = jnp.bfloat16


def dot(left, right):
    return jnp.dot(left, right, preferred_element_type=F32)


def dot_t(left, right):
    return lax.dot_general(left, right, (((1,), (1,)), ((), ())), preferred_element_type=F32)


def silu(v):
    return v * (0.5 + 0.5 * jnp.tanh(0.5 * v))


def rms(values, gain):
    return values * lax.rsqrt(jnp.mean(values * values, axis=-1, keepdims=True) + 1e-06) * gain


def to_columns(row, lanes=128):
    return jnp.broadcast_to(row, (lanes, row.shape[1])).T


def kernel(
    count,
    grid_in,
    dest_block,
    dest_node,
    mask_in,
    mesh_embed,
    w_in,
    in_bias,
    w_grid,
    w_enc,
    attn_gain,
    w_query,
    w_key,
    w_value,
    w_out,
    mlp_gain,
    w_up,
    w_down,
    dec_gain,
    w_dec,
    w_head,
    w_final,
    out,
    v_grid,
    v_db,
    v_dn,
    v_mask,
    v_embed,
    v_win,
    v_bias,
    v_wgrid,
    v_wenc,
    v_again,
    v_wq,
    v_wk,
    v_wv,
    v_wo,
    v_mgain,
    v_wu,
    v_wd,
    v_dgain,
    v_wdec,
    v_whead,
    v_wfinal,
    feat,
    psend,
    csend,
    crecv,
    erecv,
    pown,
    pnear,
    state,
    bias,
    xs,
    rx,
    q_scr,
    k_scr,
    v_scr,
    m_scr,
    r_scr,
    att,
    gather,
    acc,
    obuf,
    load_sem,
    es_sem,
    er_sem,
    xs_sem,
    xr_sem,
    out_sem,
):
    me = lax.axis_index("block")
    core = lax.rem(me, 2)
    side = 2 * core - 1
    grid_rows, _ = grid_in.shape
    mesh_rows, width = mesh_embed.shape
    half = mesh_rows // HALVES

    def device(offset):
        return {"block": lax.rem(me + offset + count, count)}

    barrier = pltpu.get_barrier_semaphore()
    for offset in (-2, -1, 1, 2):
        pl.semaphore_signal(barrier, inc=1, device_id=device(offset), device_id_type=MESH)

    sources = (
        grid_in, dest_block, dest_node, w_in, in_bias, w_grid, mask_in, mesh_embed, w_enc, attn_gain,
        w_query, w_key, w_value, w_out, mlp_gain, w_up, w_down, dec_gain, w_dec, w_head, w_final,
    )
    targets = (
        v_grid, v_db, v_dn, v_win, v_bias, v_wgrid, v_mask, v_embed, v_wenc, v_again,
        v_wq, v_wk, v_wv, v_wo, v_mgain, v_wu, v_wd, v_dgain, v_wdec, v_whead, v_wfinal,
    )
    loads = {}
    for index, (source, target) in enumerate(zip(sources, targets)):
        copy = pltpu.make_async_copy(source, target, load_sem.at[index])
        copy.start()
        loads[index] = copy

    def need(*refs):
        for index, target in enumerate(targets):
            if any(target is ref for ref in refs) and index in loads:
                loads.pop(index).wait()

    started = []

    def send(src, dst, s_sem, r_sem, offset):
        copy = pltpu.make_async_remote_copy(
            src_ref=src,
            dst_ref=dst,
            send_sem=s_sem,
            recv_sem=r_sem,
            device_id=device(offset),
            device_id_type=MESH,
        )
        copy.start()
        started.append(copy)
        return copy

    need(v_grid, v_win, v_bias, v_wgrid, v_db, v_dn)
    in_row = v_bias[...].astype(F32)
    for step in range(grid_rows // mesh_rows):
        rows = pl.ds(step * mesh_rows, mesh_rows)
        hidden = silu(dot(v_grid[rows, :], v_win[...]) + in_row).astype(BF16)
        feat[rows, :] = dot(hidden, v_wgrid[...]).astype(BF16)

    relative = v_db[...] - me
    relative = jnp.where(relative > count // 2, relative - count, relative)
    relative = jnp.where(relative < -(count // 2), relative + count, relative)
    code = relative * mesh_rows + v_dn[...]
    ones = jnp.ones((8, grid_rows), BF16)

    def partial(k):
        nodes = lax.broadcasted_iota(jnp.int32, (mesh_rows, grid_rows), 0) + k * side * mesh_rows
        match = jnp.where(nodes == code, 1.0, 0.0).astype(BF16)
        return dot(match, feat[...]), dot_t(ones, match)

    hrows = [pl.ds(h * half, half) for h in range(HALVES)]
    enc = {}

    def enc_send(name, index, slot, h, offset):
        enc[name] = send(
            psend.at[slot, hrows[h], :],
            erecv.at[slot, hrows[h], :],
            es_sem.at[index],
            er_sem.at[index],
            offset,
        )

    def count_send(index, counts, offset):
        csend[index] = counts
        enc[("count", index)] = send(
            csend.at[index], crecv.at[index], es_sem.at[8 + index], er_sem.at[8 + index], offset
        )

    sums, counts = partial(-2)
    psend[0] = sums.astype(BF16)
    pl.semaphore_wait(barrier, 4)
    for h in range(HALVES):
        enc_send(("combine", h), h, 0, h, -side)
    count_send(0, counts, -2 * side)
    sums, counts = partial(2)
    psend[1] = sums.astype(BF16)
    enc_send(("far", 0), 2, 1, 0, 2 * side)
    count_send(1, counts, 2 * side)
    sums, counts = partial(1)
    pnear[...] = sums
    count_send(3, counts, side)
    for h in range(HALVES):
        enc[("combine", h)].wait_recv()
        psend[3, hrows[h], :] = (pnear[hrows[h], :] + erecv[0, hrows[h], :].astype(F32)).astype(BF16)
        enc_send(("near", h), 4 + h, 3, h, side)
        if h == 0:
            enc_send(("far", 1), 3, 1, 1, 2 * side)
    sums, counts = partial(-1)
    psend[2] = sums.astype(BF16)
    for h in range(HALVES):
        enc_send(("partner", h), 6 + h, 2, h, -side)
    count_send(2, counts, -side)
    sums, own_counts = partial(0)
    pown[...] = sums

    code_columns = to_columns(code.astype(F32))
    lane = lax.broadcasted_iota(jnp.int32, (1, mesh_rows), 1).astype(F32)
    code_wide = jnp.concatenate([code_columns, code_columns], axis=1)
    base = (side * mesh_rows).astype(F32)
    for slot, k in enumerate((0, -1, -2, 2, 1)):
        gather[slot] = jnp.where(code_wide == lane + k * base, 1.0, 0.0).astype(BF16)

    need(v_mask)
    columns = [to_columns(v_mask[pl.ds(c, 1), :].astype(F32)) for c in range(4)]
    minus = jnp.zeros((mesh_rows, 128), F32) + core.astype(F32) > 0.5
    by_slot = (
        jnp.where(minus, columns[1], columns[2]),
        jnp.where(minus, columns[0], columns[3]),
        jnp.where(minus, columns[3], columns[0]),
        jnp.where(minus, columns[2], columns[1]),
    )
    for slot, value in enumerate(by_slot):
        bias[slot] = jnp.where(value > 0.5, 0.0, BIG)

    far_sends = {}

    def broadcast(phase, h):
        for slot, offset in ((0, -side), (1, 2 * side), (2, -2 * side)):
            far_sends[phase, slot, h] = send(
                xs.at[phase, hrows[h], :],
                rx.at[phase, slot, hrows[h], :],
                xs_sem.at[phase, slot, h],
                xr_sem.at[phase, slot, h],
                offset,
            )

    def forward(phase, h):
        far_sends[phase, 1, h].wait_recv()
        far_sends[phase, 3, h] = send(
            rx.at[phase, 1, hrows[h], :],
            rx.at[phase, 3, hrows[h], :],
            xs_sem.at[phase, 3, h],
            xr_sem.at[phase, 3, h],
            -side,
        )

    need(v_embed, v_wenc, v_again)
    for index in range(4):
        enc[("count", index)].wait_recv()
    total = own_counts + crecv[0] + crecv[1] + crecv[2] + crecv[3]
    scale = to_columns(1.0 / jnp.maximum(total[0:1, :], 1.0))
    scale = jnp.concatenate([scale] * (width // 128), axis=1)
    for h in range(HALVES):
        rows = hrows[h]
        for name in ("partner", "far", "near"):
            enc[(name, h)].wait_recv()
        summed = pown[rows, :] + erecv[1, rows, :].astype(F32)
        summed = summed + erecv[2, rows, :].astype(F32) + erecv[3, rows, :].astype(F32)
        mean_rows = (summed * scale[h * half : (h + 1) * half]).astype(BF16)
        value = v_embed[rows, :].astype(F32) + dot(mean_rows, v_wenc[...])
        state[rows, :] = value
        xs[0, rows, :] = rms(value, v_again[pl.ds(0, 1), :].astype(F32)).astype(BF16)
        broadcast(0, h)

    low = lax.broadcasted_iota(jnp.int32, (1, 128), 1) < 64

    def project(layer, slot, value):
        keys = dot(value, v_wk[layer])
        values = dot(value, v_wv[layer])
        for j in range(PAIRS):
            cut = slice(j * 128, (j + 1) * 128)
            k_scr[slot, j] = keys[:, cut].astype(BF16)
            v_scr[slot, 2 * j] = jnp.where(low, values[:, cut], 1.0).astype(BF16)
            v_scr[slot, 2 * j + 1] = jnp.where(low, 1.0, values[:, cut]).astype(BF16)

    def group(h, j, rows, slots, start):
        query = q_scr[h, rows, :]
        scores = [dot_t(query, k_scr[slot, j]) for slot in slots]
        best = start
        for slot, score in zip(slots, scores):
            top = jnp.maximum(score[:, :128], score[:, 128:])
            if slot:
                top = top - bias[slot - 1, rows, :]
            best = top if best is None else jnp.maximum(best, top)
        best = jnp.broadcast_to(jnp.max(best, axis=-1, keepdims=True), best.shape)
        result = None
        for slot, score in zip(slots, scores):
            shift = best + bias[slot - 1, rows, :] if slot else best
            weights = jnp.exp(score - jnp.concatenate([shift, shift], axis=1)).astype(BF16)
            term = dot(weights, v_scr[slot, h])
            result = term if result is None else result + term
        return best, result

    for layer in range(LAYERS):
        need(v_wq, v_wk, v_wv)
        value = xs[layer]
        queries = dot(value, v_wq[layer]) * 0.125
        for j in range(PAIRS):
            cut = queries[:, j * 128 : (j + 1) * 128]
            q_scr[2 * j] = jnp.where(low, cut, 0.0).astype(BF16)
            q_scr[2 * j + 1] = jnp.where(low, 0.0, cut).astype(BF16)
        project(layer, 0, value)
        for h in range(HALVES):
            far_sends[layer, 0, h].wait_recv()
        project(layer, 1, rx[layer, 0])
        everything = pl.ds(0, mesh_rows)

        def first(h):
            for odd in range(2):
                best, result = group(2 * h + odd, h, everything, (0, 1), None)
                m_scr[2 * h + odd] = best
                r_scr[2 * h + odd] = result

        for j in range(PAIRS):
            first(j)
            if j % 2 == 1:
                forward(layer, j // 2)
        for slot in (1, 2, 3):
            for h in range(HALVES):
                if slot > 1:
                    far_sends[layer, slot, h].wait_recv()
            project(layer, slot + 1, rx[layer, slot])
        need(v_wo, v_mgain, v_wu, v_wd, v_dgain, v_wdec)
        for h in range(HALVES):
            rows = hrows[h]
            for j in range(PAIRS):
                parts = []
                for odd in range(2):
                    head = 2 * j + odd
                    before = m_scr[head, rows, :]
                    best, result = group(head, j, rows, (2, 3, 4), before)
                    parts.append(r_scr[head, rows, :] * jnp.exp(before - best) + result)
                top = jnp.where(low, parts[0], parts[1])
                bottom = pltpu.roll(jnp.where(low, parts[1], parts[0]), 64, 1)
                att[rows, pl.ds(j * 128, 128)] = (top / bottom).astype(BF16)
            value = state[rows, :] + dot(att[rows, :], v_wo[layer])
            normed = rms(value, v_mgain[pl.ds(layer, 1), :].astype(F32)).astype(BF16)
            up = silu(dot(normed, v_wu[layer])).astype(BF16)
            value = value + dot(up, v_wd[layer])
            if layer + 1 < LAYERS:
                state[rows, :] = value
                sent = rms(value, v_again[pl.ds(layer + 1, 1), :].astype(F32)).astype(BF16)
            else:
                decoded = rms(value, v_dgain[...].astype(F32)).astype(BF16)
                sent = dot(decoded, v_wdec[...]).astype(BF16)
            xs[layer + 1, rows, :] = sent
            broadcast(layer + 1, h)

    steps = grid_rows // mesh_rows
    for h in range(HALVES):
        far_sends[LAYERS, 0, h].wait_recv()
    for step in range(steps):
        rows = pl.ds(step * mesh_rows, mesh_rows)
        acc[rows, :] = (
            feat[rows, :].astype(F32)
            + dot(gather[0, rows, :], xs[LAYERS])
            + dot(gather[1, rows, :], rx[LAYERS, 0])
        )
        if step % 2 == 1:
            forward(LAYERS, step // 2)
    for h in range(HALVES):
        far_sends[LAYERS, 2, h].wait_recv()
    for step in range(steps):
        rows = pl.ds(step * mesh_rows, mesh_rows)
        acc[rows, :] = (
            acc[rows, :]
            + dot(gather[2, rows, :], rx[LAYERS, 1])
            + dot(gather[3, rows, :], rx[LAYERS, 2])
        )
    for h in range(HALVES):
        far_sends[LAYERS, 3, h].wait_recv()
    need(v_whead, v_wfinal)
    writes = []
    for step in range(steps):
        rows = pl.ds(step * mesh_rows, mesh_rows)
        mixed = (acc[rows, :] + dot(gather[4, rows, :], rx[LAYERS, 3])).astype(BF16)
        head_rows = silu(dot(mixed, v_whead[...])).astype(BF16)
        obuf[rows, :] = dot(head_rows, v_wfinal[...]).astype(BF16)
        copy = pltpu.make_async_copy(obuf.at[rows, :], out.at[rows, :], out_sem.at[step])
        copy.start()
        writes.append(copy)
    for copy in started:
        copy.wait_send()
    for copy in writes:
        copy.wait()


def body(
    grid_in, dest_block, dest_node, neighbour_mask, mesh_embed, w_in, in_bias, w_grid, w_enc, attn_gain,
    w_query, w_key, w_value, w_out, mlp_gain, w_up, w_down, dec_gain, w_dec, w_head, w_final,
):
    count = lax.axis_size("block")
    grid_rows, channels = grid_in.shape
    mesh_rows, width = mesh_embed.shape
    operands = [
        grid_in,
        dest_block.reshape(1, grid_rows),
        dest_node.reshape(1, grid_rows),
        neighbour_mask.T,
        mesh_embed,
        w_in,
        in_bias.reshape(1, width),
        w_grid,
        w_enc,
        attn_gain,
        w_query,
        w_key,
        w_value,
        w_out,
        mlp_gain,
        w_up,
        w_down,
        dec_gain.reshape(1, width),
        w_dec,
        w_head,
        w_final,
    ]
    phases = LAYERS + 1
    scratch = [pltpu.VMEM(operand.shape, operand.dtype) for operand in operands] + [
        pltpu.VMEM((grid_rows, width), BF16),
        pltpu.VMEM((4, mesh_rows, width), BF16),
        pltpu.VMEM((4, 8, mesh_rows), F32),
        pltpu.VMEM((4, 8, mesh_rows), F32),
        pltpu.VMEM((4, mesh_rows, width), BF16),
        pltpu.VMEM((mesh_rows, width), F32),
        pltpu.VMEM((mesh_rows, width), F32),
        pltpu.VMEM((mesh_rows, width), F32),
        pltpu.VMEM((4, mesh_rows, 128), F32),
        pltpu.VMEM((phases, mesh_rows, width), BF16),
        pltpu.VMEM((phases, 4, mesh_rows, width), BF16),
        pltpu.VMEM((HEADS, mesh_rows, 128), BF16),
        pltpu.VMEM((5, PAIRS, mesh_rows, 128), BF16),
        pltpu.VMEM((5, HEADS, mesh_rows, 128), BF16),
        pltpu.VMEM((HEADS, mesh_rows, 128), F32),
        pltpu.VMEM((HEADS, mesh_rows, 128), F32),
        pltpu.VMEM((mesh_rows, width), BF16),
        pltpu.VMEM((5, grid_rows, mesh_rows), BF16),
        pltpu.VMEM((grid_rows, width), F32),
        pltpu.VMEM((grid_rows, channels), BF16),
        pltpu.SemaphoreType.DMA((len(operands),)),
        pltpu.SemaphoreType.DMA((12,)),
        pltpu.SemaphoreType.DMA((12,)),
        pltpu.SemaphoreType.DMA((phases, 4, HALVES)),
        pltpu.SemaphoreType.DMA((phases, 4, HALVES)),
        pltpu.SemaphoreType.DMA((grid_rows // mesh_rows,)),
    ]
    return pl.pallas_call(
        functools.partial(kernel, count),
        out_shape=jax.ShapeDtypeStruct((grid_rows, channels), BF16),
        in_specs=[pl.BlockSpec(memory_space=pl.ANY)] * len(operands),
        out_specs=pl.BlockSpec(memory_space=pl.ANY),
        scratch_shapes=scratch,
        compiler_params=pltpu.CompilerParams(
            collective_id=0, has_side_effects=True, vmem_limit_bytes=60 * 1024 * 1024
        ),
        name="step",
    )(*operands)


def solution(mesh):
    rows = P(("member", "block"), None)
    placed = (rows, rows, P(("member", "block")), rows, rows) + (P(),) * 16
    return jax.shard_map(body, mesh=mesh, in_specs=placed, out_specs=rows, check_vma=False)
```

```python
import functools

import jax
import jax.numpy as jnp
from jax import lax
from jax.experimental import pallas as pl
from jax.experimental.pallas import tpu as pltpu
from jax.sharding import PartitionSpec as P

HEADS = 8
LAYERS = 2
PAIRS = HEADS // 2
HALVES = 2
BIG = 1e30
MESH = pl.DeviceIdType.MESH
F32 = jnp.float32
BF16 = jnp.bfloat16


def dot(left, right):
    return jnp.dot(left, right, preferred_element_type=F32)


def dot_t(left, right):
    return lax.dot_general(left, right, (((1,), (1,)), ((), ())), preferred_element_type=F32)


def silu(v):
    return v * (0.5 + 0.5 * jnp.tanh(0.5 * v))


def rms(values, gain):
    return values * lax.rsqrt(jnp.mean(values * values, axis=-1, keepdims=True) + 1e-06) * gain


def as_row(ref):
    value = ref[...].astype(F32)
    return jnp.concatenate([value[i : i + 1] for i in range(value.shape[0])], axis=1)


def to_columns(row, lanes=128):
    return jnp.broadcast_to(row, (lanes, row.shape[1])).T


def kernel(
    count,
    grid_in,
    dest_block,
    dest_node,
    mask_in,
    mesh_embed,
    w_in,
    in_bias,
    w_grid,
    w_enc,
    attn_gain,
    w_query,
    w_key,
    w_value,
    w_out,
    mlp_gain,
    w_up,
    w_down,
    dec_gain,
    w_dec,
    w_head,
    w_final,
    out,
    v_grid,
    v_db,
    v_dn,
    v_mask,
    v_embed,
    v_win,
    v_bias,
    v_wgrid,
    v_wenc,
    v_again,
    v_wq,
    v_wk,
    v_wv,
    v_wo,
    v_mgain,
    v_wu,
    v_wd,
    v_dgain,
    v_wdec,
    v_whead,
    v_wfinal,
    feat,
    psend,
    csend,
    crecv,
    erecv,
    pown,
    pnear,
    state,
    bias,
    xs,
    rx,
    q_scr,
    k_scr,
    v_scr,
    m_scr,
    r_scr,
    att,
    gather,
    acc,
    load_sem,
    es_sem,
    er_sem,
    xs_sem,
    xr_sem,
):
    me = lax.axis_index("block")
    core = lax.rem(me, 2)
    side = 2 * core - 1
    grid_rows, _ = grid_in.shape
    mesh_rows, width = mesh_embed.shape
    half = mesh_rows // HALVES

    def device(offset):
        return {"block": lax.rem(me + offset + count, count)}

    barrier = pltpu.get_barrier_semaphore()
    for offset in (-2, -1, 1, 2):
        pl.semaphore_signal(barrier, inc=1, device_id=device(offset), device_id_type=MESH)

    sources = (
        grid_in, dest_block, dest_node, w_in, in_bias, w_grid, mask_in, mesh_embed, w_enc, attn_gain,
        w_query, w_key, w_value, w_out, mlp_gain, w_up, w_down, dec_gain, w_dec, w_head, w_final,
    )
    targets = (
        v_grid, v_db, v_dn, v_win, v_bias, v_wgrid, v_mask, v_embed, v_wenc, v_again,
        v_wq, v_wk, v_wv, v_wo, v_mgain, v_wu, v_wd, v_dgain, v_wdec, v_whead, v_wfinal,
    )
    loads = {}

    def load(first, last):
        for index in range(first, last):
            copy = pltpu.make_async_copy(sources[index], targets[index], load_sem.at[index])
            copy.start()
            loads[index] = copy

    load(0, 6)

    def need(*refs):
        for index, target in enumerate(targets):
            if any(target is ref for ref in refs) and index in loads:
                loads.pop(index).wait()

    started = []

    def send(src, dst, s_sem, r_sem, offset):
        copy = pltpu.make_async_remote_copy(
            src_ref=src,
            dst_ref=dst,
            send_sem=s_sem,
            recv_sem=r_sem,
            device_id=device(offset),
            device_id_type=MESH,
        )
        copy.start()
        started.append(copy)
        return copy

    need(v_grid, v_win, v_bias, v_wgrid, v_db, v_dn)
    load(6, len(sources))
    in_row = as_row(v_bias)
    for step in range(grid_rows // mesh_rows):
        rows = pl.ds(step * mesh_rows, mesh_rows)
        hidden = silu(dot(v_grid[rows, :], v_win[...]) + in_row).astype(BF16)
        feat[rows, :] = dot(hidden, v_wgrid[...]).astype(BF16)

    relative = v_db[...] - me
    relative = jnp.where(relative > count // 2, relative - count, relative)
    relative = jnp.where(relative < -(count // 2), relative + count, relative)
    code = relative * mesh_rows + v_dn[...]
    ones = jnp.ones((8, grid_rows), BF16)

    def partial(k):
        nodes = lax.broadcasted_iota(jnp.int32, (mesh_rows, grid_rows), 0) + k * side * mesh_rows
        match = jnp.where(nodes == code, 1.0, 0.0).astype(BF16)
        return dot(match, feat[...]), dot_t(ones, match)

    hrows = [pl.ds(h * half, half) for h in range(HALVES)]
    enc = {}

    def enc_send(name, index, slot, h, offset):
        enc[name] = send(
            psend.at[slot, hrows[h], :],
            erecv.at[slot, hrows[h], :],
            es_sem.at[index],
            er_sem.at[index],
            offset,
        )

    def count_send(index, counts, offset):
        csend[index] = counts
        enc[("count", index)] = send(
            csend.at[index], crecv.at[index], es_sem.at[8 + index], er_sem.at[8 + index], offset
        )

    sums, counts = partial(-2)
    psend[0] = sums.astype(BF16)
    pl.semaphore_wait(barrier, 4)
    for h in range(HALVES):
        enc_send(("combine", h), h, 0, h, -side)
    count_send(0, counts, -2 * side)
    sums, counts = partial(2)
    psend[1] = sums.astype(BF16)
    enc_send(("far", 0), 2, 1, 0, 2 * side)
    count_send(1, counts, 2 * side)
    sums, counts = partial(1)
    pnear[...] = sums
    count_send(3, counts, side)
    for h in range(HALVES):
        enc[("combine", h)].wait_recv()
        psend[3, hrows[h], :] = (pnear[hrows[h], :] + erecv[0, hrows[h], :].astype(F32)).astype(BF16)
        enc_send(("near", h), 4 + h, 3, h, side)
        if h == 0:
            enc_send(("far", 1), 3, 1, 1, 2 * side)
    sums, counts = partial(-1)
    psend[2] = sums.astype(BF16)
    for h in range(HALVES):
        enc_send(("partner", h), 6 + h, 2, h, -side)
    count_send(2, counts, -side)
    sums, own_counts = partial(0)
    pown[...] = sums

    code_columns = to_columns(code.astype(F32))
    lane = lax.broadcasted_iota(jnp.int32, (1, mesh_rows), 1).astype(F32)
    code_wide = jnp.concatenate([code_columns, code_columns], axis=1)
    base = (side * mesh_rows).astype(F32)
    left = lane < half
    wanted = (
        lane,
        lane - base,
        lane - 2 * base,
        jnp.where(left, lane + 2 * base, lane - half + base),
        jnp.where(left, lane + half + 2 * base, lane + base),
    )
    for tile, node in enumerate(wanted):
        gather[tile] = jnp.where(code_wide == node, 1.0, 0.0).astype(BF16)

    need(v_mask)
    columns = [to_columns(v_mask[pl.ds(c, 1), :].astype(F32)) for c in range(4)]
    minus = jnp.zeros((mesh_rows, 128), F32) + core.astype(F32) > 0.5
    by_slot = (
        jnp.where(minus, columns[1], columns[2]),
        jnp.where(minus, columns[0], columns[3]),
        jnp.where(minus, columns[3], columns[0]),
        jnp.where(minus, columns[2], columns[1]),
    )
    for slot, value in enumerate(by_slot):
        bias[slot] = jnp.where(value > 0.5, 0.0, BIG)

    far_sends = {}

    tile_rows = (pl.ds(0, half), pl.ds(half, half))

    def far_send(phase, name, h, source, slot, rows, offset):
        index = ("partner", "ahead", "behind", "passed").index(name)
        far_sends[phase, name, h] = send(
            source,
            rx.at[phase, slot, rows, :],
            xs_sem.at[phase, index, h],
            xr_sem.at[phase, index, h],
            offset,
        )

    def broadcast(phase, h):
        source = xs.at[phase, hrows[h], :]
        far_send(phase, "ahead", h, source, 1, hrows[h], 2 * side)
        far_send(phase, "partner", h, source, 0, hrows[h], -side)

    def rest(phase, h):
        far_send(phase, "behind", h, xs.at[phase, hrows[h], :], 2 + h, tile_rows[0], -2 * side)

    def forward(phase, h):
        far_sends[phase, "ahead", h].wait_recv()
        far_send(phase, "passed", h, rx.at[phase, 1, hrows[h], :], 2 + h, tile_rows[1], -side)

    def arrived(phase, name, *parts):
        for h in parts:
            far_sends[phase, name, h].wait_recv()

    need(v_embed, v_wenc, v_again)
    for index in range(4):
        enc[("count", index)].wait_recv()
    total = own_counts + crecv[0] + crecv[1] + crecv[2] + crecv[3]
    scale = to_columns(1.0 / jnp.maximum(total[0:1, :], 1.0))
    scale = jnp.concatenate([scale] * (width // 128), axis=1)
    for h in range(HALVES):
        rows = hrows[h]
        for name in ("partner", "far", "near"):
            enc[(name, h)].wait_recv()
        summed = pown[rows, :] + erecv[1, rows, :].astype(F32)
        summed = summed + erecv[2, rows, :].astype(F32) + erecv[3, rows, :].astype(F32)
        mean_rows = (summed * scale[h * half : (h + 1) * half]).astype(BF16)
        value = v_embed[rows, :].astype(F32) + dot(mean_rows, v_wenc[...])
        state[rows, :] = value
        xs[0, rows, :] = rms(value, v_again[pl.ds(0, 1), :].astype(F32)).astype(BF16)
        broadcast(0, h)
    rest(0, 0)

    low = lax.broadcasted_iota(jnp.int32, (1, 128), 1) < 64

    def project(layer, slot, value):
        keys = dot(value, v_wk[layer])
        values = dot(value, v_wv[layer])
        for j in range(PAIRS):
            cut = slice(j * 128, (j + 1) * 128)
            k_scr[slot, j] = keys[:, cut].astype(BF16)
            v_scr[slot, 2 * j] = jnp.where(low, values[:, cut], 1.0).astype(BF16)
            v_scr[slot, 2 * j + 1] = jnp.where(low, 1.0, values[:, cut]).astype(BF16)

    mask_of = {1: (0, 0), 2: (1, 1), 3: (2, 3), 4: (2, 3)}

    def group(head, rows, tiles, start):
        query = q_scr[head, rows, :]
        scores = [dot_t(query, k_scr[tile, head // 2]) for tile in tiles]
        best = start
        for tile, score in zip(tiles, scores):
            sides = [score[:, :128], score[:, 128:]]
            if tile and mask_of[tile][0] == mask_of[tile][1]:
                top = jnp.maximum(*sides) - bias[mask_of[tile][0], rows, :]
            elif tile:
                top = jnp.maximum(*(x - bias[m, rows, :] for x, m in zip(sides, mask_of[tile])))
            else:
                top = jnp.maximum(*sides)
            best = top if best is None else jnp.maximum(best, top)
        best = jnp.broadcast_to(jnp.max(best, axis=-1, keepdims=True), best.shape)
        result = None
        for tile, score in zip(tiles, scores):
            if tile:
                shift = jnp.concatenate([best + bias[m, rows, :] for m in mask_of[tile]], axis=1)
            else:
                shift = jnp.concatenate([best, best], axis=1)
            weights = jnp.exp(score - shift).astype(BF16)
            term = dot(weights, v_scr[tile, head])
            result = term if result is None else result + term
        return best, result

    def merged(head, rows, tiles):
        before = m_scr[head, rows, :]
        best, result = group(head, rows, tiles, before)
        return best, r_scr[head, rows, :] * jnp.exp(before - best) + result

    everything = pl.ds(0, mesh_rows)

    def absorb(tile):
        for head in range(HEADS):
            best, result = merged(head, everything, (tile,))
            m_scr[head] = best
            r_scr[head] = result

    for layer in range(LAYERS):
        need(v_wq, v_wk, v_wv)
        value = xs[layer]
        queries = dot(value, v_wq[layer]) * 0.125
        for j in range(PAIRS):
            cut = queries[:, j * 128 : (j + 1) * 128]
            q_scr[2 * j] = jnp.where(low, cut, 0.0).astype(BF16)
            q_scr[2 * j + 1] = jnp.where(low, 0.0, cut).astype(BF16)
        project(layer, 0, value)
        arrived(layer, "partner", 0, 1)
        project(layer, 1, rx[layer, 0])
        for head in range(HEADS):
            best, result = group(head, everything, (0, 1), None)
            m_scr[head] = best
            r_scr[head] = result
            if head == 5:
                forward(layer, 0)
                rest(layer, 1)
        arrived(layer, "behind", 0)
        arrived(layer, "passed", 0)
        project(layer, 3, rx[layer, 2])
        absorb(3)
        forward(layer, 1)
        project(layer, 2, rx[layer, 1])
        absorb(2)
        arrived(layer, "behind", 1)
        arrived(layer, "passed", 1)
        project(layer, 4, rx[layer, 3])
        need(v_wo, v_mgain, v_wu, v_wd, v_dgain, v_wdec)
        for h in range(HALVES):
            rows = hrows[h]
            for j in range(PAIRS):
                parts = [merged(2 * j + odd, rows, (4,))[1] for odd in range(2)]
                top = jnp.where(low, parts[0], parts[1])
                bottom = pltpu.roll(jnp.where(low, parts[1], parts[0]), 64, 1)
                att[rows, pl.ds(j * 128, 128)] = (top / bottom).astype(BF16)
            if h:
                rest(layer + 1, 0)
            value = state[rows, :] + dot(att[rows, :], v_wo[layer])
            normed = rms(value, v_mgain[pl.ds(layer, 1), :].astype(F32)).astype(BF16)
            up = silu(dot(normed, v_wu[layer])).astype(BF16)
            value = value + dot(up, v_wd[layer])
            if layer + 1 < LAYERS:
                state[rows, :] = value
                sent = rms(value, v_again[pl.ds(layer + 1, 1), :].astype(F32)).astype(BF16)
            else:
                decoded = rms(value, as_row(v_dgain)).astype(BF16)
                sent = dot(decoded, v_wdec[...]).astype(BF16)
            xs[layer + 1, rows, :] = sent
            broadcast(layer + 1, h)

    steps = grid_rows // mesh_rows
    last = LAYERS

    def add(tile, slot):
        for step in range(steps):
            rows = pl.ds(step * mesh_rows, mesh_rows)
            acc[rows, :] = acc[rows, :] + dot(gather[tile, rows, :], rx[last, slot])

    arrived(last, "partner", 0, 1)
    for step in range(steps):
        rows = pl.ds(step * mesh_rows, mesh_rows)
        acc[rows, :] = (
            feat[rows, :].astype(F32)
            + dot(gather[0, rows, :], xs[last])
            + dot(gather[1, rows, :], rx[last, 0])
        )
        if step == 1:
            rest(last, 1)
    forward(last, 0)
    arrived(last, "behind", 0)
    arrived(last, "passed", 0)
    add(3, 2)
    forward(last, 1)
    add(2, 1)
    need(v_whead, v_wfinal)
    arrived(last, "behind", 1)
    arrived(last, "passed", 1)
    for step in range(steps):
        rows = pl.ds(step * mesh_rows, mesh_rows)
        mixed = (acc[rows, :] + dot(gather[4, rows, :], rx[last, 3])).astype(BF16)
        head_rows = silu(dot(mixed, v_whead[...])).astype(BF16)
        out[rows, :] = dot(head_rows, v_wfinal[...]).astype(BF16)
    for copy in started:
        copy.wait_send()


def body(
    grid_in, dest_block, dest_node, neighbour_mask, mesh_embed, w_in, in_bias, w_grid, w_enc, attn_gain,
    w_query, w_key, w_value, w_out, mlp_gain, w_up, w_down, dec_gain, w_dec, w_head, w_final,
):
    count = lax.axis_size("block")
    grid_rows, channels = grid_in.shape
    mesh_rows, width = mesh_embed.shape
    operands = [
        grid_in,
        dest_block.reshape(1, grid_rows),
        dest_node.reshape(1, grid_rows),
        neighbour_mask.T,
        mesh_embed,
        w_in,
        in_bias.reshape(width // 128, 128),
        w_grid,
        w_enc,
        attn_gain,
        w_query,
        w_key,
        w_value,
        w_out,
        mlp_gain,
        w_up,
        w_down,
        dec_gain.reshape(width // 128, 128),
        w_dec,
        w_head,
        w_final,
    ]
    phases = LAYERS + 1
    scratch = [pltpu.VMEM(operand.shape, operand.dtype) for operand in operands] + [
        pltpu.VMEM((grid_rows, width), BF16),
        pltpu.VMEM((4, mesh_rows, width), BF16),
        pltpu.VMEM((4, 8, mesh_rows), F32),
        pltpu.VMEM((4, 8, mesh_rows), F32),
        pltpu.VMEM((4, mesh_rows, width), BF16),
        pltpu.VMEM((mesh_rows, width), F32),
        pltpu.VMEM((mesh_rows, width), F32),
        pltpu.VMEM((mesh_rows, width), F32),
        pltpu.VMEM((4, mesh_rows, 128), F32),
        pltpu.VMEM((phases, mesh_rows, width), BF16),
        pltpu.VMEM((phases, 4, mesh_rows, width), BF16),
        pltpu.VMEM((HEADS, mesh_rows, 128), BF16),
        pltpu.VMEM((5, PAIRS, mesh_rows, 128), BF16),
        pltpu.VMEM((5, HEADS, mesh_rows, 128), BF16),
        pltpu.VMEM((HEADS, mesh_rows, 128), F32),
        pltpu.VMEM((HEADS, mesh_rows, 128), F32),
        pltpu.VMEM((mesh_rows, width), BF16),
        pltpu.VMEM((5, grid_rows, mesh_rows), BF16),
        pltpu.VMEM((grid_rows, width), F32),
        pltpu.SemaphoreType.DMA((len(operands),)),
        pltpu.SemaphoreType.DMA((12,)),
        pltpu.SemaphoreType.DMA((12,)),
        pltpu.SemaphoreType.DMA((phases, 4, HALVES)),
        pltpu.SemaphoreType.DMA((phases, 4, HALVES)),
    ]
    return pl.pallas_call(
        functools.partial(kernel, count),
        out_shape=jax.ShapeDtypeStruct((grid_rows, channels), BF16),
        in_specs=[pl.BlockSpec(memory_space=pl.ANY)] * len(operands),
        out_specs=pl.BlockSpec(memory_space=pltpu.VMEM),
        scratch_shapes=scratch,
        compiler_params=pltpu.CompilerParams(
            collective_id=0, has_side_effects=True, vmem_limit_bytes=60 * 1024 * 1024
        ),
        name="step",
    )(*operands)


def solution(mesh):
    rows = P(("member", "block"), None)
    placed = (rows, rows, P(("member", "block")), rows, rows) + (P(),) * 16
    return jax.shard_map(body, mesh=mesh, in_specs=placed, out_specs=rows, check_vma=False)
```

```python
import functools

import jax
import jax.numpy as jnp
from jax import lax
from jax.experimental import pallas as pl
from jax.experimental.pallas import tpu as pltpu
from jax.sharding import PartitionSpec as P

HEADS = 8
LAYERS = 2
PAIRS = HEADS // 2
HALVES = 2
BIG = 1e30
LOG2E = 1.4426950408889634
MESH = pl.DeviceIdType.MESH
F32 = jnp.float32
BF16 = jnp.bfloat16


def dot(left, right):
    return jnp.dot(left, right, preferred_element_type=F32)


def dot_t(left, right):
    return lax.dot_general(left, right, (((1,), (1,)), ((), ())), preferred_element_type=F32)


def silu(v):
    return v * (0.5 + 0.5 * jnp.tanh(0.5 * v))


def rms(values, gain):
    return values * lax.rsqrt(jnp.mean(values * values, axis=-1, keepdims=True) + 1e-06) * gain


def as_row(ref):
    value = ref[...].astype(F32)
    return jnp.concatenate([value[i : i + 1] for i in range(value.shape[0])], axis=1)


def to_columns(row, lanes=128):
    return jnp.broadcast_to(row, (lanes, row.shape[1])).T


def kernel(
    count,
    grid_in,
    dest_block,
    dest_node,
    mask_in,
    mesh_embed,
    w_in,
    in_bias,
    w_grid,
    w_enc,
    attn_gain,
    w_query,
    w_key,
    w_value,
    w_out,
    mlp_gain,
    w_up,
    w_down,
    dec_gain,
    w_dec,
    w_head,
    w_final,
    out,
    v_grid,
    v_db,
    v_dn,
    v_mask,
    v_embed,
    v_win,
    v_bias,
    v_wgrid,
    v_wenc,
    v_again,
    v_wq,
    v_wk,
    v_wv,
    v_wo,
    v_mgain,
    v_wu,
    v_wd,
    v_dgain,
    v_wdec,
    v_whead,
    v_wfinal,
    hidden,
    feat,
    psend,
    csend,
    crecv,
    erecv,
    pown,
    pnear,
    state,
    bias,
    xs,
    rx,
    q_scr,
    k_scr,
    v_scr,
    m_scr,
    r_scr,
    att,
    gather,
    acc,
    load_sem,
    es_sem,
    er_sem,
    xs_sem,
    xr_sem,
):
    me = lax.axis_index("block")
    core = lax.rem(me, 2)
    side = 2 * core - 1
    grid_rows, _ = grid_in.shape
    mesh_rows, width = mesh_embed.shape
    half = mesh_rows // HALVES

    def device(offset):
        return {"block": lax.rem(me + offset + count, count)}

    barrier = pltpu.get_barrier_semaphore()
    for offset in (-2, -1, 1, 2):
        pl.semaphore_signal(barrier, inc=1, device_id=device(offset), device_id_type=MESH)

    sources = (
        grid_in, dest_block, dest_node, w_in, in_bias, w_grid, mask_in, mesh_embed, w_enc, attn_gain,
        w_query, w_key, w_value, w_out, mlp_gain, w_up, w_down, dec_gain, w_dec, w_head, w_final,
    )
    targets = (
        v_grid, v_db, v_dn, v_win, v_bias, v_wgrid, v_mask, v_embed, v_wenc, v_again,
        v_wq, v_wk, v_wv, v_wo, v_mgain, v_wu, v_wd, v_dgain, v_wdec, v_whead, v_wfinal,
    )
    loads = {}

    def load(first, last):
        for index in range(first, last):
            copy = pltpu.make_async_copy(sources[index], targets[index], load_sem.at[index])
            copy.start()
            loads[index] = copy

    load(0, 5)

    def need(*refs):
        for index, target in enumerate(targets):
            if any(target is ref for ref in refs) and index in loads:
                loads.pop(index).wait()

    started = []

    def send(src, dst, s_sem, r_sem, offset):
        copy = pltpu.make_async_remote_copy(
            src_ref=src,
            dst_ref=dst,
            send_sem=s_sem,
            recv_sem=r_sem,
            device_id=device(offset),
            device_id_type=MESH,
        )
        copy.start()
        started.append(copy)
        return copy

    need(v_grid, v_win, v_bias, v_db, v_dn)
    load(5, len(sources))
    in_row = as_row(v_bias)
    for step in range(grid_rows // mesh_rows):
        rows = pl.ds(step * mesh_rows, mesh_rows)
        hidden[rows, :] = silu(dot(v_grid[rows, :], v_win[...]) + in_row).astype(BF16)

    relative = v_db[...] - me
    relative = jnp.where(relative > count // 2, relative - count, relative)
    relative = jnp.where(relative < -(count // 2), relative + count, relative)
    code = relative * mesh_rows + v_dn[...]
    ones = jnp.ones((8, grid_rows), BF16)

    def partial(k):
        nodes = lax.broadcasted_iota(jnp.int32, (mesh_rows, grid_rows), 0) + k * side * mesh_rows
        match = jnp.where(nodes == code, 1.0, 0.0).astype(BF16)
        return dot(match, hidden[...]), dot_t(ones, match)

    hrows = [pl.ds(h * half, half) for h in range(HALVES)]
    enc = {}

    def enc_send(name, index, slot, h, offset):
        enc[name] = send(
            psend.at[slot, hrows[h], :],
            erecv.at[slot, hrows[h], :],
            es_sem.at[index],
            er_sem.at[index],
            offset,
        )

    def count_send(index, counts, offset):
        csend[index] = counts
        enc[("count", index)] = send(
            csend.at[index], crecv.at[index], es_sem.at[8 + index], er_sem.at[8 + index], offset
        )

    sums, counts = partial(-2)
    psend[0] = sums.astype(BF16)
    pl.semaphore_wait(barrier, 4)
    for h in range(HALVES):
        enc_send(("combine", h), h, 0, h, -side)
    count_send(0, counts, -2 * side)
    sums, counts = partial(2)
    psend[1] = sums.astype(BF16)
    enc_send(("far", 0), 2, 1, 0, 2 * side)
    count_send(1, counts, 2 * side)
    sums, counts = partial(1)
    pnear[...] = sums
    count_send(3, counts, side)
    for h in range(HALVES):
        enc[("combine", h)].wait_recv()
        psend[3, hrows[h], :] = (pnear[hrows[h], :] + erecv[0, hrows[h], :].astype(F32)).astype(BF16)
        enc_send(("near", h), 4 + h, 3, h, side)
        if h == 0:
            enc_send(("far", 1), 3, 1, 1, 2 * side)
    sums, counts = partial(-1)
    psend[2] = sums.astype(BF16)
    for h in range(HALVES):
        enc_send(("partner", h), 6 + h, 2, h, -side)
    count_send(2, counts, -side)
    sums, own_counts = partial(0)
    pown[...] = sums

    need(v_wgrid)
    for step in range(grid_rows // mesh_rows):
        rows = pl.ds(step * mesh_rows, mesh_rows)
        feat[rows, :] = dot(hidden[rows, :], v_wgrid[...]).astype(BF16)

    code_columns = to_columns(code.astype(F32))
    lane = lax.broadcasted_iota(jnp.int32, (1, mesh_rows), 1).astype(F32)
    code_wide = jnp.concatenate([code_columns, code_columns], axis=1)
    base = (side * mesh_rows).astype(F32)
    left = lane < half
    wanted = (
        lane,
        lane - base,
        lane - 2 * base,
        jnp.where(left, lane + 2 * base, lane - half + base),
        jnp.where(left, lane + half + 2 * base, lane + base),
    )
    for tile, node in enumerate(wanted):
        gather[tile] = jnp.where(code_wide == node, 1.0, 0.0).astype(BF16)

    need(v_mask)
    columns = [to_columns(v_mask[pl.ds(c, 1), :].astype(F32)) for c in range(4)]
    minus = jnp.zeros((mesh_rows, 128), F32) + core.astype(F32) > 0.5
    by_slot = (
        jnp.where(minus, columns[1], columns[2]),
        jnp.where(minus, columns[0], columns[3]),
        jnp.where(minus, columns[3], columns[0]),
        jnp.where(minus, columns[2], columns[1]),
    )
    lane_wide = lax.broadcasted_iota(jnp.int32, (1, 128), 1)
    low = lane_wide < 64

    def tag(odd, kind):
        return jnp.where(lane_wide == kind + (0 if odd else 64), 1.0, 0.0)

    for odd in range(2):
        total = jnp.zeros((mesh_rows, 128), F32)
        for kind, value in enumerate(by_slot):
            total = total + jnp.where(value > 0.5, 0.0, -BIG) * tag(odd, kind)
        bias[odd] = total

    far_sends = {}

    tile_rows = (pl.ds(0, half), pl.ds(half, half))

    def far_send(phase, name, h, source, slot, rows, offset):
        index = ("partner", "ahead", "behind", "passed").index(name)
        far_sends[phase, name, h] = send(
            source,
            rx.at[phase, slot, rows, :],
            xs_sem.at[phase, index, h],
            xr_sem.at[phase, index, h],
            offset,
        )

    def broadcast(phase, h):
        source = xs.at[phase, hrows[h], :]
        far_send(phase, "ahead", h, source, 1, hrows[h], 2 * side)
        far_send(phase, "partner", h, source, 0, hrows[h], -side)

    def rest(phase, h):
        far_send(phase, "behind", h, xs.at[phase, hrows[h], :], 2 + h, tile_rows[0], -2 * side)

    def forward(phase, h):
        far_sends[phase, "ahead", h].wait_recv()
        far_send(phase, "passed", h, rx.at[phase, 1, hrows[h], :], 2 + h, tile_rows[1], -side)

    def arrived(phase, name, *parts):
        for h in parts:
            far_sends[phase, name, h].wait_recv()

    need(v_embed, v_wenc, v_again)
    for index in range(4):
        enc[("count", index)].wait_recv()
    total = own_counts + crecv[0] + crecv[1] + crecv[2] + crecv[3]
    scale = to_columns(1.0 / jnp.maximum(total[0:1, :], 1.0))
    scale = jnp.concatenate([scale] * (width // 128), axis=1)
    for h in range(HALVES):
        rows = hrows[h]
        for name in ("partner", "far", "near"):
            enc[(name, h)].wait_recv()
        summed = pown[rows, :] + erecv[1, rows, :].astype(F32)
        summed = summed + erecv[2, rows, :].astype(F32) + erecv[3, rows, :].astype(F32)
        mean_hidden = (summed * scale[h * half : (h + 1) * half]).astype(BF16)
        mean_rows = dot(mean_hidden, v_wgrid[...]).astype(BF16)
        value = v_embed[rows, :].astype(F32) + dot(mean_rows, v_wenc[...])
        state[rows, :] = value
        xs[0, rows, :] = rms(value, v_again[pl.ds(0, 1), :].astype(F32)).astype(BF16)
        broadcast(0, h)
    rest(0, 0)

    def project(layer, tile, value):
        keys = dot(value, v_wk[layer])
        values = dot(value, v_wv[layer])
        for head in range(HEADS):
            odd = head % 2
            cut = slice(head // 2 * 128, (head // 2 + 1) * 128)
            k_cut, v_cut = keys[:, cut], values[:, cut]
            mine = low if odd == 0 else jnp.logical_not(low)
            v_scr[tile, head] = jnp.where(mine, v_cut, 1.0).astype(BF16)
            if tile < 3:
                other = tag(odd, tile - 1) if tile else 0.0
                k_scr[tile, head] = jnp.where(mine, k_cut, other).astype(BF16)
            else:
                for part in range(HALVES):
                    part_rows = slice(part * half, (part + 1) * half)
                    k_scr[tile, head, pl.ds(part * half, half), :] = jnp.where(
                        mine, k_cut[part_rows], tag(odd, 2 + part)
                    ).astype(BF16)

    def group(head, rows, tiles, start):
        query = q_scr[head, rows, :]
        scores = [dot_t(query, k_scr[tile, head]) for tile in tiles]
        best = start
        for score in scores:
            top = jnp.maximum(score[:, :128], score[:, 128:])
            best = top if best is None else jnp.maximum(best, top)
        best = jnp.broadcast_to(jnp.max(best, axis=-1, keepdims=True), best.shape)
        shift = jnp.concatenate([best, best], axis=1)
        result = None
        for tile, score in zip(tiles, scores):
            term = dot(jnp.exp2(score - shift).astype(BF16), v_scr[tile, head])
            result = term if result is None else result + term
        return best, result

    def merged(head, rows, tiles):
        before = m_scr[head, rows, :]
        best, result = group(head, rows, tiles, before)
        return best, r_scr[head, rows, :] * jnp.exp2(before - best) + result

    everything = pl.ds(0, mesh_rows)

    def absorb(tile):
        for head in range(HEADS):
            best, result = merged(head, everything, (tile,))
            m_scr[head] = best
            r_scr[head] = result

    for layer in range(LAYERS):
        need(v_wq, v_wk, v_wv)
        value = xs[layer]
        queries = dot(value, v_wq[layer]) * (0.125 * LOG2E)
        for j in range(PAIRS):
            cut = queries[:, j * 128 : (j + 1) * 128]
            q_scr[2 * j] = jnp.where(low, cut, bias[0]).astype(BF16)
            q_scr[2 * j + 1] = jnp.where(low, bias[1], cut).astype(BF16)
        project(layer, 0, value)
        arrived(layer, "partner", 0, 1)
        project(layer, 1, rx[layer, 0])
        for head in range(HEADS):
            best, result = group(head, everything, (0, 1), None)
            m_scr[head] = best
            r_scr[head] = result
            if head == 5:
                forward(layer, 0)
                rest(layer, 1)
        arrived(layer, "behind", 0)
        arrived(layer, "passed", 0)
        project(layer, 3, rx[layer, 2])
        absorb(3)
        forward(layer, 1)
        project(layer, 2, rx[layer, 1])
        absorb(2)
        arrived(layer, "behind", 1)
        arrived(layer, "passed", 1)
        project(layer, 4, rx[layer, 3])
        need(v_wo, v_mgain, v_wu, v_wd, v_dgain, v_wdec)
        for h in range(HALVES):
            rows = hrows[h]
            for j in range(PAIRS):
                parts = [merged(2 * j + odd, rows, (4,))[1] for odd in range(2)]
                top = jnp.where(low, parts[0], parts[1])
                bottom = pltpu.roll(jnp.where(low, parts[1], parts[0]), 64, 1)
                att[rows, pl.ds(j * 128, 128)] = (top / bottom).astype(BF16)
            if h:
                rest(layer + 1, 0)
            value = state[rows, :] + dot(att[rows, :], v_wo[layer])
            normed = rms(value, v_mgain[pl.ds(layer, 1), :].astype(F32)).astype(BF16)
            up = silu(dot(normed, v_wu[layer])).astype(BF16)
            value = value + dot(up, v_wd[layer])
            if layer + 1 < LAYERS:
                state[rows, :] = value
                sent = rms(value, v_again[pl.ds(layer + 1, 1), :].astype(F32)).astype(BF16)
            else:
                decoded = rms(value, as_row(v_dgain)).astype(BF16)
                sent = dot(decoded, v_wdec[...]).astype(BF16)
            xs[layer + 1, rows, :] = sent
            broadcast(layer + 1, h)

    steps = grid_rows // mesh_rows
    last = LAYERS

    def add(tile, slot):
        for step in range(steps):
            rows = pl.ds(step * mesh_rows, mesh_rows)
            acc[rows, :] = acc[rows, :] + dot(gather[tile, rows, :], rx[last, slot])

    arrived(last, "partner", 0, 1)
    for step in range(steps):
        rows = pl.ds(step * mesh_rows, mesh_rows)
        acc[rows, :] = (
            feat[rows, :].astype(F32)
            + dot(gather[0, rows, :], xs[last])
            + dot(gather[1, rows, :], rx[last, 0])
        )
        if step == 1:
            rest(last, 1)
    forward(last, 0)
    arrived(last, "behind", 0)
    arrived(last, "passed", 0)
    add(3, 2)
    forward(last, 1)
    add(2, 1)
    need(v_whead, v_wfinal)
    arrived(last, "behind", 1)
    arrived(last, "passed", 1)
    for step in range(steps):
        rows = pl.ds(step * mesh_rows, mesh_rows)
        mixed = (acc[rows, :] + dot(gather[4, rows, :], rx[last, 3])).astype(BF16)
        head_rows = silu(dot(mixed, v_whead[...])).astype(BF16)
        out[rows, :] = dot(head_rows, v_wfinal[...]).astype(BF16)
    for copy in started:
        copy.wait_send()


def body(
    grid_in, dest_block, dest_node, neighbour_mask, mesh_embed, w_in, in_bias, w_grid, w_enc, attn_gain,
    w_query, w_key, w_value, w_out, mlp_gain, w_up, w_down, dec_gain, w_dec, w_head, w_final,
):
    count = lax.axis_size("block")
    grid_rows, channels = grid_in.shape
    mesh_rows, width = mesh_embed.shape
    operands = [
        grid_in,
        dest_block.reshape(1, grid_rows),
        dest_node.reshape(1, grid_rows),
        neighbour_mask.T,
        mesh_embed,
        w_in,
        in_bias.reshape(width // 128, 128),
        w_grid,
        w_enc,
        attn_gain,
        w_query,
        w_key,
        w_value,
        w_out,
        mlp_gain,
        w_up,
        w_down,
        dec_gain.reshape(width // 128, 128),
        w_dec,
        w_head,
        w_final,
    ]
    phases = LAYERS + 1
    scratch = [pltpu.VMEM(operand.shape, operand.dtype) for operand in operands] + [
        pltpu.VMEM((grid_rows, width), BF16),
        pltpu.VMEM((grid_rows, width), BF16),
        pltpu.VMEM((4, mesh_rows, width), BF16),
        pltpu.VMEM((4, 8, mesh_rows), F32),
        pltpu.VMEM((4, 8, mesh_rows), F32),
        pltpu.VMEM((4, mesh_rows, width), BF16),
        pltpu.VMEM((mesh_rows, width), F32),
        pltpu.VMEM((mesh_rows, width), F32),
        pltpu.VMEM((mesh_rows, width), F32),
        pltpu.VMEM((2, mesh_rows, 128), F32),
        pltpu.VMEM((phases, mesh_rows, width), BF16),
        pltpu.VMEM((phases, 4, mesh_rows, width), BF16),
        pltpu.VMEM((HEADS, mesh_rows, 128), BF16),
        pltpu.VMEM((5, HEADS, mesh_rows, 128), BF16),
        pltpu.VMEM((5, HEADS, mesh_rows, 128), BF16),
        pltpu.VMEM((HEADS, mesh_rows, 128), F32),
        pltpu.VMEM((HEADS, mesh_rows, 128), F32),
        pltpu.VMEM((mesh_rows, width), BF16),
        pltpu.VMEM((5, grid_rows, mesh_rows), BF16),
        pltpu.VMEM((grid_rows, width), F32),
        pltpu.SemaphoreType.DMA((len(operands),)),
        pltpu.SemaphoreType.DMA((12,)),
        pltpu.SemaphoreType.DMA((12,)),
        pltpu.SemaphoreType.DMA((phases, 4, HALVES)),
        pltpu.SemaphoreType.DMA((phases, 4, HALVES)),
    ]
    return pl.pallas_call(
        functools.partial(kernel, count),
        out_shape=pltpu.VMEM((grid_rows, channels), BF16),
        in_specs=[pl.BlockSpec(memory_space=pl.ANY)] * len(operands),
        out_specs=pl.BlockSpec(memory_space=pltpu.VMEM),
        scratch_shapes=scratch,
        compiler_params=pltpu.CompilerParams(
            collective_id=0, has_side_effects=True, vmem_limit_bytes=60 * 1024 * 1024
        ),
        name="step",
    )(*operands)


def solution(mesh):
    rows = P(("member", "block"), None)
    placed = (rows, rows, P(("member", "block")), rows, rows) + (P(),) * 16
    return jax.shard_map(body, mesh=mesh, in_specs=placed, out_specs=rows, check_vma=False)
```

```python
import functools

import jax
import jax.numpy as jnp
from jax import lax
from jax.experimental import pallas as pl
from jax.experimental.pallas import tpu as pltpu
from jax.sharding import PartitionSpec as P

HEADS = 8
LAYERS = 2
PAIRS = HEADS // 2
HALVES = 2
BIG = 1e30
LOG2E = 1.4426950408889634
MESH = pl.DeviceIdType.MESH
F32 = jnp.float32
BF16 = jnp.bfloat16


def dot(left, right):
    return jnp.dot(left, right, preferred_element_type=F32)


def dot_t(left, right):
    return lax.dot_general(left, right, (((1,), (1,)), ((), ())), preferred_element_type=F32)


def silu(v):
    return v * (0.5 + 0.5 * jnp.tanh(0.5 * v))


def rms(values, gain):
    return values * lax.rsqrt(jnp.mean(values * values, axis=-1, keepdims=True) + 1e-06) * gain


def as_row(ref):
    value = ref[...].astype(F32)
    return jnp.concatenate([value[i : i + 1] for i in range(value.shape[0])], axis=1)


def to_columns(row, lanes=128):
    return jnp.broadcast_to(row, (lanes, row.shape[1])).T


def kernel(
    count,
    grid_in,
    dest_block,
    dest_node,
    mask_in,
    mesh_embed,
    w_in,
    in_bias,
    w_grid,
    w_enc,
    attn_gain,
    w_query,
    w_key,
    w_value,
    w_out,
    mlp_gain,
    w_up,
    w_down,
    dec_gain,
    w_dec,
    w_head,
    w_final,
    out,
    v_grid,
    v_db,
    v_dn,
    v_mask,
    v_embed,
    v_win,
    v_bias,
    v_wgrid,
    v_wenc,
    v_again,
    v_wq,
    v_wk,
    v_wv,
    v_wo,
    v_mgain,
    v_wu,
    v_wd,
    v_dgain,
    v_wdec,
    v_whead,
    v_wfinal,
    w_first,
    w_last,
    hidden,
    feat,
    psend,
    csend,
    crecv,
    erecv,
    pown,
    pnear,
    state,
    bias,
    xs,
    rx,
    q_scr,
    k_scr,
    v_scr,
    m_scr,
    r_scr,
    att,
    gather,
    acc,
    load_sem,
    es_sem,
    er_sem,
    xs_sem,
    xr_sem,
):
    me = lax.axis_index("block")
    core = lax.rem(me, 2)
    side = 2 * core - 1
    grid_rows, _ = grid_in.shape
    mesh_rows, width = mesh_embed.shape
    half = mesh_rows // HALVES

    def device(offset):
        return {"block": lax.rem(me + offset + count, count)}

    barrier = pltpu.get_barrier_semaphore()
    for offset in (-2, -1, 1, 2):
        pl.semaphore_signal(barrier, inc=1, device_id=device(offset), device_id_type=MESH)

    sources = (
        grid_in, dest_block, dest_node, w_in, in_bias, w_grid, mask_in, mesh_embed, w_enc, attn_gain,
        w_query, w_key, w_value, w_out, mlp_gain, w_up, w_down, dec_gain, w_dec, w_head, w_final,
    )
    targets = (
        v_grid, v_db, v_dn, v_win, v_bias, v_wgrid, v_mask, v_embed, v_wenc, v_again,
        v_wq, v_wk, v_wv, v_wo, v_mgain, v_wu, v_wd, v_dgain, v_wdec, v_whead, v_wfinal,
    )
    loads = {}

    def load(first, last):
        for index in range(first, last):
            copy = pltpu.make_async_copy(sources[index], targets[index], load_sem.at[index])
            copy.start()
            loads[index] = copy

    load(0, 5)

    def need(*refs):
        for index, target in enumerate(targets):
            if any(target is ref for ref in refs) and index in loads:
                loads.pop(index).wait()

    started = []

    def send(src, dst, s_sem, r_sem, offset):
        copy = pltpu.make_async_remote_copy(
            src_ref=src,
            dst_ref=dst,
            send_sem=s_sem,
            recv_sem=r_sem,
            device_id=device(offset),
            device_id_type=MESH,
        )
        copy.start()
        started.append(copy)
        return copy

    need(v_grid, v_win, v_bias, v_db, v_dn)
    load(5, len(sources))
    in_row = as_row(v_bias)
    for step in range(grid_rows // mesh_rows):
        rows = pl.ds(step * mesh_rows, mesh_rows)
        hidden[rows, :] = silu(dot(v_grid[rows, :], v_win[...]) + in_row).astype(BF16)

    relative = v_db[...] - me
    relative = jnp.where(relative > count // 2, relative - count, relative)
    relative = jnp.where(relative < -(count // 2), relative + count, relative)
    code = relative * mesh_rows + v_dn[...]
    ones = jnp.ones((8, grid_rows), BF16)

    def partial(k):
        nodes = lax.broadcasted_iota(jnp.int32, (mesh_rows, grid_rows), 0) + k * side * mesh_rows
        match = jnp.where(nodes == code, 1.0, 0.0).astype(BF16)
        return dot(match, hidden[...]), dot_t(ones, match)

    hrows = [pl.ds(h * half, half) for h in range(HALVES)]
    enc = {}

    def enc_send(name, index, slot, h, offset):
        enc[name] = send(
            psend.at[slot, hrows[h], :],
            erecv.at[slot, hrows[h], :],
            es_sem.at[index],
            er_sem.at[index],
            offset,
        )

    def count_send(index, counts, offset):
        csend[index] = counts
        enc[("count", index)] = send(
            csend.at[index], crecv.at[index], es_sem.at[8 + index], er_sem.at[8 + index], offset
        )

    sums, counts = partial(-2)
    psend[0] = sums.astype(BF16)
    pl.semaphore_wait(barrier, 4)
    for h in range(HALVES):
        enc_send(("combine", h), h, 0, h, -side)
    count_send(0, counts, -2 * side)
    sums, counts = partial(2)
    psend[1] = sums.astype(BF16)
    enc_send(("far", 0), 2, 1, 0, 2 * side)
    count_send(1, counts, 2 * side)
    sums, counts = partial(1)
    pnear[...] = sums
    count_send(3, counts, side)
    for h in range(HALVES):
        enc[("combine", h)].wait_recv()
        psend[3, hrows[h], :] = (pnear[hrows[h], :] + erecv[0, hrows[h], :].astype(F32)).astype(BF16)
        enc_send(("near", h), 4 + h, 3, h, side)
        if h == 0:
            enc_send(("far", 1), 3, 1, 1, 2 * side)
    sums, counts = partial(-1)
    psend[2] = sums.astype(BF16)
    for h in range(HALVES):
        enc_send(("partner", h), 6 + h, 2, h, -side)
    count_send(2, counts, -side)
    sums, own_counts = partial(0)
    pown[...] = sums

    need(v_mask)
    columns = [to_columns(v_mask[pl.ds(c, 1), :].astype(F32)) for c in range(4)]
    minus = jnp.zeros((mesh_rows, 128), F32) + core.astype(F32) > 0.5
    by_slot = (
        jnp.where(minus, columns[1], columns[2]),
        jnp.where(minus, columns[0], columns[3]),
        jnp.where(minus, columns[3], columns[0]),
        jnp.where(minus, columns[2], columns[1]),
    )
    lane_wide = lax.broadcasted_iota(jnp.int32, (1, 128), 1)
    low = lane_wide < 64

    def tag(odd, kind):
        return jnp.where(lane_wide == kind + (0 if odd else 64), 1.0, 0.0)

    for odd in range(2):
        total = jnp.zeros((mesh_rows, 128), F32)
        for kind, value in enumerate(by_slot):
            total = total + jnp.where(value > 0.5, 0.0, -BIG) * tag(odd, kind)
        bias[odd] = total

    def product(target, left, right):
        for step in range(width // mesh_rows):
            rows = pl.ds(step * mesh_rows, mesh_rows)
            target[rows, :] = dot(left[rows, :], right[...]).astype(BF16)

    need(v_wgrid, v_wenc, v_wdec, v_whead)
    product(w_first, v_wgrid, v_wenc)
    product(w_last, v_wdec, v_whead)

    far_sends = {}

    tile_rows = (pl.ds(0, half), pl.ds(half, half))

    def far_send(phase, name, h, source, slot, rows, offset):
        index = ("partner", "ahead", "behind", "passed").index(name)
        far_sends[phase, name, h] = send(
            source,
            rx.at[phase, slot, rows, :],
            xs_sem.at[phase, index, h],
            xr_sem.at[phase, index, h],
            offset,
        )

    def broadcast(phase, h):
        source = xs.at[phase, hrows[h], :]
        far_send(phase, "ahead", h, source, 1, hrows[h], 2 * side)
        far_send(phase, "partner", h, source, 0, hrows[h], -side)

    def rest(phase, h):
        far_send(phase, "behind", h, xs.at[phase, hrows[h], :], 2 + h, tile_rows[0], -2 * side)

    def forward(phase, h):
        far_sends[phase, "ahead", h].wait_recv()
        far_send(phase, "passed", h, rx.at[phase, 1, hrows[h], :], 2 + h, tile_rows[1], -side)

    def arrived(phase, name, *parts):
        for h in parts:
            far_sends[phase, name, h].wait_recv()

    need(v_embed, v_wenc, v_again)
    for index in range(4):
        enc[("count", index)].wait_recv()
    total = own_counts + crecv[0] + crecv[1] + crecv[2] + crecv[3]
    scale = to_columns(1.0 / jnp.maximum(total[0:1, :], 1.0))
    scale = jnp.concatenate([scale] * (width // 128), axis=1)
    for h in range(HALVES):
        rows = hrows[h]
        for name in ("partner", "far", "near"):
            enc[(name, h)].wait_recv()
        summed = pown[rows, :] + erecv[1, rows, :].astype(F32)
        summed = summed + erecv[2, rows, :].astype(F32) + erecv[3, rows, :].astype(F32)
        mean_hidden = (summed * scale[h * half : (h + 1) * half]).astype(BF16)
        value = v_embed[rows, :].astype(F32) + dot(mean_hidden, w_first[...])
        state[rows, :] = value
        xs[0, rows, :] = rms(value, v_again[pl.ds(0, 1), :].astype(F32)).astype(BF16)
        broadcast(0, h)
    rest(0, 0)

    def project(layer, tile, value):
        keys = dot(value, v_wk[layer])
        values = dot(value, v_wv[layer])
        for head in range(HEADS):
            odd = head % 2
            cut = slice(head // 2 * 128, (head // 2 + 1) * 128)
            k_cut, v_cut = keys[:, cut], values[:, cut]
            mine = low if odd == 0 else jnp.logical_not(low)
            v_scr[tile, head] = jnp.where(mine, v_cut, 1.0).astype(BF16)
            if tile < 3:
                other = tag(odd, tile - 1) if tile else 0.0
                k_scr[tile, head] = jnp.where(mine, k_cut, other).astype(BF16)
            else:
                for part in range(HALVES):
                    part_rows = slice(part * half, (part + 1) * half)
                    k_scr[tile, head, pl.ds(part * half, half), :] = jnp.where(
                        mine, k_cut[part_rows], tag(odd, 2 + part)
                    ).astype(BF16)

    def score_all(head, rows, tiles):
        query = q_scr[head, rows, :]
        return [dot_t(query, k_scr[tile, head]) for tile in tiles]

    def soften(head, tiles, scores, start):
        best = start
        for score in scores:
            top = jnp.maximum(score[:, :128], score[:, 128:])
            best = top if best is None else jnp.maximum(best, top)
        best = jnp.broadcast_to(jnp.max(best, axis=-1, keepdims=True), best.shape)
        shift = jnp.concatenate([best, best], axis=1)
        result = None
        for tile, score in zip(tiles, scores):
            term = dot(jnp.exp2(score - shift).astype(BF16), v_scr[tile, head])
            result = term if result is None else result + term
        return best, result

    def attention(rows, tiles, fresh, consume):
        coming = score_all(0, rows, tiles)
        for head in range(HEADS):
            scores = coming
            if head + 1 < HEADS:
                coming = score_all(head + 1, rows, tiles)
            before = None if fresh else m_scr[head, rows, :]
            best, result = soften(head, tiles, scores, before)
            if not fresh:
                result = r_scr[head, rows, :] * jnp.exp2(before - best) + result
            consume(head, best, result)

    everything = pl.ds(0, mesh_rows)

    def keep(head, best, result):
        m_scr[head] = best
        r_scr[head] = result

    def absorb(tile):
        attention(everything, (tile,), False, keep)

    for layer in range(LAYERS):
        need(v_wq, v_wk, v_wv)
        value = xs[layer]
        queries = dot(value, v_wq[layer]) * (0.125 * LOG2E)
        for j in range(PAIRS):
            cut = queries[:, j * 128 : (j + 1) * 128]
            q_scr[2 * j] = jnp.where(low, cut, bias[0]).astype(BF16)
            q_scr[2 * j + 1] = jnp.where(low, bias[1], cut).astype(BF16)
        project(layer, 0, value)
        arrived(layer, "partner", 0, 1)
        project(layer, 1, rx[layer, 0])

        def keep_first(head, best, result):
            keep(head, best, result)
            if head == 5:
                forward(layer, 0)
                rest(layer, 1)

        attention(everything, (0, 1), True, keep_first)
        arrived(layer, "behind", 0)
        arrived(layer, "passed", 0)
        project(layer, 3, rx[layer, 2])
        absorb(3)
        forward(layer, 1)
        project(layer, 2, rx[layer, 1])
        absorb(2)
        arrived(layer, "behind", 1)
        arrived(layer, "passed", 1)
        project(layer, 4, rx[layer, 3])
        need(v_wo, v_mgain, v_wu, v_wd, v_dgain)

        def stages(h, layer=layer):
            rows = hrows[h]
            value = state[rows, :] + dot(att[rows, :], v_wo[layer])
            normed = rms(value, v_mgain[pl.ds(layer, 1), :].astype(F32)).astype(BF16)
            yield
            up = silu(dot(normed, v_wu[layer])).astype(BF16)
            yield
            value = value + dot(up, v_wd[layer])
            if layer + 1 < LAYERS:
                state[rows, :] = value
                sent = rms(value, v_again[pl.ds(layer + 1, 1), :].astype(F32)).astype(BF16)
            else:
                decoded = rms(value, as_row(v_dgain)).astype(BF16)
                yield
                sent = dot(decoded, w_last[...]).astype(BF16)
            xs[layer + 1, rows, :] = sent
            broadcast(layer + 1, h)

        running = iter(())
        for h in range(HALVES):
            parts = {}

            def finish(head, best, result, rows=hrows[h], parts=parts, running=running):
                parts[head % 2] = result
                if head % 2:
                    top = jnp.where(low, parts[0], parts[1])
                    bottom = pltpu.roll(jnp.where(low, parts[1], parts[0]), 64, 1)
                    att[rows, pl.ds(head // 2 * 128, 128)] = (top / bottom).astype(BF16)
                next(running, None)

            attention(hrows[h], (4,), False, finish)
            running = stages(h)
            next(running, None)
        rest(layer + 1, 0)
        for _ in running:
            pass

    steps = grid_rows // mesh_rows
    last = LAYERS

    def add(tile, slot):
        for step in range(steps):
            rows = pl.ds(step * mesh_rows, mesh_rows)
            acc[rows, :] = acc[rows, :] + dot(gather[tile, rows, :], rx[last, slot])

    code_columns = to_columns(code.astype(F32))
    lane = lax.broadcasted_iota(jnp.int32, (1, mesh_rows), 1).astype(F32)
    code_wide = jnp.concatenate([code_columns, code_columns], axis=1)
    base = (side * mesh_rows).astype(F32)
    left = lane < half
    wanted = (
        lane,
        lane - base,
        lane - 2 * base,
        jnp.where(left, lane + 2 * base, lane - half + base),
        jnp.where(left, lane + half + 2 * base, lane + base),
    )
    for tile, node in enumerate(wanted):
        gather[tile] = jnp.where(code_wide == node, 1.0, 0.0).astype(BF16)

    for step in range(steps):
        rows = pl.ds(step * mesh_rows, mesh_rows)
        feat[rows, :] = dot(hidden[rows, :], v_wgrid[...]).astype(BF16)
    arrived(last, "partner", 0, 1)
    for step in range(steps):
        rows = pl.ds(step * mesh_rows, mesh_rows)
        acc[rows, :] = (
            dot(feat[rows, :], v_whead[...])
            + dot(gather[0, rows, :], xs[last])
            + dot(gather[1, rows, :], rx[last, 0])
        )
        if step == 1:
            rest(last, 1)
    forward(last, 0)
    arrived(last, "behind", 0)
    arrived(last, "passed", 0)
    add(3, 2)
    forward(last, 1)
    add(2, 1)
    need(v_wfinal)
    arrived(last, "behind", 1)
    arrived(last, "passed", 1)
    for step in range(steps):
        rows = pl.ds(step * mesh_rows, mesh_rows)
        head_rows = silu(acc[rows, :] + dot(gather[4, rows, :], rx[last, 3])).astype(BF16)
        out[rows, :] = dot(head_rows, v_wfinal[...]).astype(BF16)
    for copy in started:
        copy.wait_send()


def body(
    grid_in, dest_block, dest_node, neighbour_mask, mesh_embed, w_in, in_bias, w_grid, w_enc, attn_gain,
    w_query, w_key, w_value, w_out, mlp_gain, w_up, w_down, dec_gain, w_dec, w_head, w_final,
):
    count = lax.axis_size("block")
    grid_rows, channels = grid_in.shape
    mesh_rows, width = mesh_embed.shape
    operands = [
        grid_in,
        dest_block.reshape(1, grid_rows),
        dest_node.reshape(1, grid_rows),
        neighbour_mask.T,
        mesh_embed,
        w_in,
        in_bias.reshape(width // 128, 128),
        w_grid,
        w_enc,
        attn_gain,
        w_query,
        w_key,
        w_value,
        w_out,
        mlp_gain,
        w_up,
        w_down,
        dec_gain.reshape(width // 128, 128),
        w_dec,
        w_head,
        w_final,
    ]
    phases = LAYERS + 1
    scratch = [pltpu.VMEM(operand.shape, operand.dtype) for operand in operands] + [
        pltpu.VMEM((width, width), BF16),
        pltpu.VMEM((width, width), BF16),
        pltpu.VMEM((grid_rows, width), BF16),
        pltpu.VMEM((grid_rows, width), BF16),
        pltpu.VMEM((4, mesh_rows, width), BF16),
        pltpu.VMEM((4, 8, mesh_rows), F32),
        pltpu.VMEM((4, 8, mesh_rows), F32),
        pltpu.VMEM((4, mesh_rows, width), BF16),
        pltpu.VMEM((mesh_rows, width), F32),
        pltpu.VMEM((mesh_rows, width), F32),
        pltpu.VMEM((mesh_rows, width), F32),
        pltpu.VMEM((2, mesh_rows, 128), F32),
        pltpu.VMEM((phases, mesh_rows, width), BF16),
        pltpu.VMEM((phases, 4, mesh_rows, width), BF16),
        pltpu.VMEM((HEADS, mesh_rows, 128), BF16),
        pltpu.VMEM((5, HEADS, mesh_rows, 128), BF16),
        pltpu.VMEM((5, HEADS, mesh_rows, 128), BF16),
        pltpu.VMEM((HEADS, mesh_rows, 128), F32),
        pltpu.VMEM((HEADS, mesh_rows, 128), F32),
        pltpu.VMEM((mesh_rows, width), BF16),
        pltpu.VMEM((5, grid_rows, mesh_rows), BF16),
        pltpu.VMEM((grid_rows, width), F32),
        pltpu.SemaphoreType.DMA((len(operands),)),
        pltpu.SemaphoreType.DMA((12,)),
        pltpu.SemaphoreType.DMA((12,)),
        pltpu.SemaphoreType.DMA((phases, 4, HALVES)),
        pltpu.SemaphoreType.DMA((phases, 4, HALVES)),
    ]
    return pl.pallas_call(
        functools.partial(kernel, count),
        out_shape=pltpu.VMEM((grid_rows, channels), BF16),
        in_specs=[pl.BlockSpec(memory_space=pl.ANY)] * len(operands),
        out_specs=pl.BlockSpec(memory_space=pltpu.VMEM),
        scratch_shapes=scratch,
        compiler_params=pltpu.CompilerParams(
            collective_id=0, has_side_effects=True, vmem_limit_bytes=60 * 1024 * 1024
        ),
        name="step",
    )(*operands)


def solution(mesh):
    rows = P(("member", "block"), None)
    placed = (rows, rows, P(("member", "block")), rows, rows) + (P(),) * 16
    return jax.shard_map(body, mesh=mesh, in_specs=placed, out_specs=rows, check_vma=False)
```

```python
import functools

import jax
import jax.numpy as jnp
from jax import lax
from jax.experimental import pallas as pl
from jax.experimental.pallas import tpu as pltpu
from jax.sharding import PartitionSpec as P

HEADS = 8
LAYERS = 2
PAIRS = HEADS // 2
HALVES = 2
BIG = 1e30
LOG2E = 1.4426950408889634
MESH = pl.DeviceIdType.MESH
F32 = jnp.float32
BF16 = jnp.bfloat16


def dot(left, right):
    return jnp.dot(left, right, preferred_element_type=F32)


def dot_t(left, right):
    return lax.dot_general(left, right, (((1,), (1,)), ((), ())), preferred_element_type=F32)


def silu(v):
    return v * (0.5 + 0.5 * jnp.tanh(0.5 * v))


def rms(values, gain):
    return values * lax.rsqrt(jnp.mean(values * values, axis=-1, keepdims=True) + 1e-06) * gain


def as_row(ref):
    value = ref[...].astype(F32)
    return jnp.concatenate([value[i : i + 1] for i in range(value.shape[0])], axis=1)


def to_columns(row, lanes=128):
    return jnp.broadcast_to(row, (lanes, row.shape[1])).T


def kernel(
    count,
    grid_in,
    dest_block,
    dest_node,
    mask_in,
    mesh_embed,
    w_in,
    in_bias,
    w_grid,
    w_enc,
    attn_gain,
    w_query,
    w_key,
    w_value,
    w_out,
    mlp_gain,
    w_up,
    w_down,
    dec_gain,
    w_dec,
    w_head,
    w_final,
    out,
    v_grid,
    v_db,
    v_dn,
    v_mask,
    v_embed,
    v_win,
    v_bias,
    v_wgrid,
    v_wenc,
    v_again,
    v_wq,
    v_wk,
    v_wv,
    v_wo,
    v_mgain,
    v_wu,
    v_wd,
    v_dgain,
    v_wdec,
    v_whead,
    v_wfinal,
    w_first,
    w_last,
    hidden,
    feat,
    psend,
    csend,
    crecv,
    erecv,
    pown,
    pnear,
    state,
    bias,
    xs,
    rx,
    q_scr,
    k_scr,
    v_scr,
    m_scr,
    r_scr,
    att,
    gather,
    acc,
    load_sem,
    es_sem,
    er_sem,
    xs_sem,
    xr_sem,
):
    me = lax.axis_index("block")
    core = lax.rem(me, 2)
    side = 2 * core - 1
    grid_rows, _ = grid_in.shape
    mesh_rows, width = mesh_embed.shape
    half = mesh_rows // HALVES

    def device(offset):
        return {"block": lax.rem(me + offset + count, count)}

    barrier = pltpu.get_barrier_semaphore()
    for offset in (-2, -1, 1, 2):
        pl.semaphore_signal(barrier, inc=1, device_id=device(offset), device_id_type=MESH)

    sources = (
        grid_in, dest_block, dest_node, w_in, in_bias, w_grid, mask_in, mesh_embed, w_enc, attn_gain,
        w_query, w_key, w_value, w_out, mlp_gain, w_up, w_down, dec_gain, w_dec, w_head, w_final,
    )
    targets = (
        v_grid, v_db, v_dn, v_win, v_bias, v_wgrid, v_mask, v_embed, v_wenc, v_again,
        v_wq, v_wk, v_wv, v_wo, v_mgain, v_wu, v_wd, v_dgain, v_wdec, v_whead, v_wfinal,
    )
    loads = {}

    def load(first, last):
        for index in range(first, last):
            copy = pltpu.make_async_copy(sources[index], targets[index], load_sem.at[index])
            copy.start()
            loads[index] = copy

    load(0, 5)

    def need(*refs):
        for index, target in enumerate(targets):
            if any(target is ref for ref in refs) and index in loads:
                loads.pop(index).wait()

    started = []

    def send(src, dst, s_sem, r_sem, offset):
        copy = pltpu.make_async_remote_copy(
            src_ref=src,
            dst_ref=dst,
            send_sem=s_sem,
            recv_sem=r_sem,
            device_id=device(offset),
            device_id_type=MESH,
        )
        copy.start()
        started.append(copy)
        return copy

    need(v_grid, v_win, v_bias, v_db, v_dn)
    load(5, len(sources))
    in_row = as_row(v_bias)
    for step in range(grid_rows // mesh_rows):
        rows = pl.ds(step * mesh_rows, mesh_rows)
        hidden[rows, :] = silu(dot(v_grid[rows, :], v_win[...]) + in_row).astype(BF16)

    relative = v_db[...] - me
    relative = jnp.where(relative > count // 2, relative - count, relative)
    relative = jnp.where(relative < -(count // 2), relative + count, relative)
    code = relative * mesh_rows + v_dn[...]
    ones = jnp.ones((8, grid_rows), BF16)

    def partial(k):
        nodes = lax.broadcasted_iota(jnp.int32, (mesh_rows, grid_rows), 0) + k * side * mesh_rows
        match = jnp.where(nodes == code, 1.0, 0.0).astype(BF16)
        return dot(match, hidden[...]), dot_t(ones, match)

    hrows = [pl.ds(h * half, half) for h in range(HALVES)]
    enc = {}

    def enc_send(name, index, slot, h, offset):
        enc[name] = send(
            psend.at[slot, hrows[h], :],
            erecv.at[slot, hrows[h], :],
            es_sem.at[index],
            er_sem.at[index],
            offset,
        )

    def count_send(index, counts, offset):
        csend[index] = counts
        enc[("count", index)] = send(
            csend.at[index], crecv.at[index], es_sem.at[8 + index], er_sem.at[8 + index], offset
        )

    sums, counts = partial(-2)
    psend[0] = sums.astype(BF16)
    pl.semaphore_wait(barrier, 4)
    for h in range(HALVES):
        enc_send(("combine", h), h, 0, h, -side)
    count_send(0, counts, -2 * side)
    sums, counts = partial(2)
    psend[1] = sums.astype(BF16)
    enc_send(("far", 0), 2, 1, 0, 2 * side)
    count_send(1, counts, 2 * side)
    sums, counts = partial(1)
    pnear[...] = sums
    count_send(3, counts, side)
    for h in range(HALVES):
        enc[("combine", h)].wait_recv()
        psend[3, hrows[h], :] = (pnear[hrows[h], :] + erecv[0, hrows[h], :].astype(F32)).astype(BF16)
        enc_send(("near", h), 4 + h, 3, h, side)
        if h == 0:
            enc_send(("far", 1), 3, 1, 1, 2 * side)
    sums, counts = partial(-1)
    psend[2] = sums.astype(BF16)
    for h in range(HALVES):
        enc_send(("partner", h), 6 + h, 2, h, -side)
    count_send(2, counts, -side)
    sums, own_counts = partial(0)
    pown[...] = sums

    need(v_mask)
    columns = [to_columns(v_mask[pl.ds(c, 1), :].astype(F32)) for c in range(4)]
    minus = jnp.zeros((mesh_rows, 128), F32) + core.astype(F32) > 0.5
    by_slot = (
        jnp.where(minus, columns[1], columns[2]),
        jnp.where(minus, columns[0], columns[3]),
        jnp.where(minus, columns[3], columns[0]),
        jnp.where(minus, columns[2], columns[1]),
    )
    lane_wide = lax.broadcasted_iota(jnp.int32, (1, 128), 1)
    low = lane_wide < 64

    def tag(odd, kind):
        return jnp.where(lane_wide == kind + (0 if odd else 64), 1.0, 0.0)

    for odd in range(2):
        total = jnp.zeros((mesh_rows, 128), F32)
        for kind, value in enumerate(by_slot):
            total = total + jnp.where(value > 0.5, 0.0, -BIG) * tag(odd, kind)
        bias[odd] = total

    def product(target, left, right):
        for step in range(width // mesh_rows):
            rows = pl.ds(step * mesh_rows, mesh_rows)
            target[rows, :] = dot(left[rows, :], right[...]).astype(BF16)

    need(v_wgrid, v_wenc, v_wdec, v_whead)
    product(w_first, v_wgrid, v_wenc)
    product(w_last, v_wdec, v_whead)

    far_sends = {}

    tile_rows = (pl.ds(0, half), pl.ds(half, half))

    def far_send(phase, name, h, source, slot, rows, offset):
        index = ("partner", "ahead", "behind", "passed").index(name)
        far_sends[phase, name, h] = send(
            source,
            rx.at[phase, slot, rows, :],
            xs_sem.at[phase, index, h],
            xr_sem.at[phase, index, h],
            offset,
        )

    def broadcast(phase, h):
        source = xs.at[phase, hrows[h], :]
        far_send(phase, "ahead", h, source, 1, hrows[h], 2 * side)
        far_send(phase, "partner", h, source, 0, hrows[h], -side)

    def rest(phase, h):
        far_send(phase, "behind", h, xs.at[phase, hrows[h], :], 2 + h, tile_rows[0], -2 * side)

    def forward(phase, h):
        far_sends[phase, "ahead", h].wait_recv()
        far_send(phase, "passed", h, rx.at[phase, 1, hrows[h], :], 2 + h, tile_rows[1], -side)

    def arrived(phase, name, *parts):
        for h in parts:
            far_sends[phase, name, h].wait_recv()

    need(v_embed, v_wenc, v_again)
    for index in range(4):
        enc[("count", index)].wait_recv()
    total = own_counts + crecv[0] + crecv[1] + crecv[2] + crecv[3]
    scale = to_columns(1.0 / jnp.maximum(total[0:1, :], 1.0))
    scale = jnp.concatenate([scale] * (width // 128), axis=1)
    for h in range(HALVES):
        rows = hrows[h]
        for name in ("partner", "far", "near"):
            enc[(name, h)].wait_recv()
        summed = pown[rows, :] + erecv[1, rows, :].astype(F32)
        summed = summed + erecv[2, rows, :].astype(F32) + erecv[3, rows, :].astype(F32)
        mean_hidden = (summed * scale[h * half : (h + 1) * half]).astype(BF16)
        value = v_embed[rows, :].astype(F32) + dot(mean_hidden, w_first[...])
        state[rows, :] = value
        xs[0, rows, :] = rms(value, v_again[pl.ds(0, 1), :].astype(F32)).astype(BF16)
        broadcast(0, h)
    rest(0, 0)

    def project(layer, tile, value):
        keys = dot(value, v_wk[layer])
        values = dot(value, v_wv[layer])
        for head in range(HEADS):
            odd = head % 2
            cut = slice(head // 2 * 128, (head // 2 + 1) * 128)
            k_cut, v_cut = keys[:, cut], values[:, cut]
            mine = low if odd == 0 else jnp.logical_not(low)
            v_scr[tile, head] = jnp.where(mine, v_cut, 1.0).astype(BF16)
            if tile < 3:
                other = tag(odd, tile - 1) if tile else 0.0
                k_scr[tile, head] = jnp.where(mine, k_cut, other).astype(BF16)
            else:
                for part in range(HALVES):
                    part_rows = slice(part * half, (part + 1) * half)
                    k_scr[tile, head, pl.ds(part * half, half), :] = jnp.where(
                        mine, k_cut[part_rows], tag(odd, 2 + part)
                    ).astype(BF16)

    def score_all(head, rows, tiles):
        query = q_scr[head, rows, :]
        return [dot_t(query, k_scr[tile, head]) for tile in tiles]

    def soften(scores, start):
        best = start
        for score in scores:
            top = jnp.maximum(score[:, :128], score[:, 128:])
            best = top if best is None else jnp.maximum(best, top)
        best = jnp.broadcast_to(jnp.max(best, axis=-1, keepdims=True), best.shape)
        shift = jnp.concatenate([best, best], axis=1)
        return best, [jnp.exp2(score - shift).astype(BF16) for score in scores]

    def attention(rows, tiles, fresh, consume):
        def close(head, before, best, weights):
            result = None
            for tile, weight in zip(tiles, weights):
                term = dot(weight, v_scr[tile, head])
                result = term if result is None else result + term
            if not fresh:
                result = r_scr[head, rows, :] * jnp.exp2(before - best) + result
            consume(head, best, result)

        coming = score_all(0, rows, tiles)
        held = None
        for head in range(HEADS):
            scores = coming
            if head + 1 < HEADS:
                coming = score_all(head + 1, rows, tiles)
            before = None if fresh else m_scr[head, rows, :]
            best, weights = soften(scores, before)
            if held is not None:
                close(*held)
            held = (head, before, best, weights)
        close(*held)

    everything = pl.ds(0, mesh_rows)

    def keep(head, best, result):
        m_scr[head] = best
        r_scr[head] = result

    def absorb(tile, after=None):
        def keep_some(head, best, result):
            keep(head, best, result)
            if head == 3 and after is not None:
                after()

        attention(everything, (tile,), False, keep_some)

    for layer in range(LAYERS):
        need(v_wq, v_wk, v_wv)
        value = xs[layer]
        queries = dot(value, v_wq[layer]) * (0.125 * LOG2E)
        for j in range(PAIRS):
            cut = queries[:, j * 128 : (j + 1) * 128]
            q_scr[2 * j] = jnp.where(low, cut, bias[0]).astype(BF16)
            q_scr[2 * j + 1] = jnp.where(low, bias[1], cut).astype(BF16)
        project(layer, 0, value)
        arrived(layer, "partner", 0, 1)
        project(layer, 1, rx[layer, 0])

        def keep_first(head, best, result):
            keep(head, best, result)
            if head == 5:
                forward(layer, 0)
                rest(layer, 1)

        attention(everything, (0, 1), True, keep_first)
        arrived(layer, "behind", 0)
        arrived(layer, "passed", 0)
        project(layer, 3, rx[layer, 2])
        absorb(3, functools.partial(forward, layer, 1))
        project(layer, 2, rx[layer, 1])
        absorb(2)
        arrived(layer, "behind", 1)
        arrived(layer, "passed", 1)
        project(layer, 4, rx[layer, 3])
        need(v_wo, v_mgain, v_wu, v_wd, v_dgain)

        def stages(h, layer=layer):
            rows = hrows[h]
            value = state[rows, :] + dot(att[rows, :], v_wo[layer])
            normed = rms(value, v_mgain[pl.ds(layer, 1), :].astype(F32)).astype(BF16)
            yield
            up = silu(dot(normed, v_wu[layer])).astype(BF16)
            yield
            value = value + dot(up, v_wd[layer])
            if layer + 1 < LAYERS:
                state[rows, :] = value
                sent = rms(value, v_again[pl.ds(layer + 1, 1), :].astype(F32)).astype(BF16)
            else:
                decoded = rms(value, as_row(v_dgain)).astype(BF16)
                yield
                sent = dot(decoded, w_last[...]).astype(BF16)
            xs[layer + 1, rows, :] = sent
            broadcast(layer + 1, h)

        running = iter(())
        for h in range(HALVES):
            parts = {}

            def finish(head, best, result, rows=hrows[h], parts=parts, running=running):
                parts[head % 2] = result
                if head % 2:
                    top = jnp.where(low, parts[0], parts[1])
                    bottom = pltpu.roll(jnp.where(low, parts[1], parts[0]), 64, 1)
                    att[rows, pl.ds(head // 2 * 128, 128)] = (top / bottom).astype(BF16)
                next(running, None)

            attention(hrows[h], (4,), False, finish)
            running = stages(h)
            next(running, None)
        rest(layer + 1, 0)
        for _ in running:
            pass

    steps = grid_rows // mesh_rows
    last = LAYERS

    def add(tile, slot):
        for step in range(steps):
            rows = pl.ds(step * mesh_rows, mesh_rows)
            acc[rows, :] = acc[rows, :] + dot(gather[tile, rows, :], rx[last, slot])

    code_columns = to_columns(code.astype(F32))
    lane = lax.broadcasted_iota(jnp.int32, (1, mesh_rows), 1).astype(F32)
    code_wide = jnp.concatenate([code_columns, code_columns], axis=1)
    base = (side * mesh_rows).astype(F32)
    left = lane < half
    wanted = (
        lane,
        lane - base,
        lane - 2 * base,
        jnp.where(left, lane + 2 * base, lane - half + base),
        jnp.where(left, lane + half + 2 * base, lane + base),
    )
    for tile, node in enumerate(wanted):
        gather[tile] = jnp.where(code_wide == node, 1.0, 0.0).astype(BF16)

    for step in range(steps):
        rows = pl.ds(step * mesh_rows, mesh_rows)
        feat[rows, :] = dot(hidden[rows, :], v_wgrid[...]).astype(BF16)
    arrived(last, "partner", 0, 1)
    for step in range(steps):
        rows = pl.ds(step * mesh_rows, mesh_rows)
        acc[rows, :] = (
            dot(feat[rows, :], v_whead[...])
            + dot(gather[0, rows, :], xs[last])
            + dot(gather[1, rows, :], rx[last, 0])
        )
        if step == 1:
            rest(last, 1)
    forward(last, 0)
    arrived(last, "behind", 0)
    arrived(last, "passed", 0)
    add(3, 2)
    forward(last, 1)
    add(2, 1)
    need(v_wfinal)
    arrived(last, "behind", 1)
    arrived(last, "passed", 1)
    for step in range(steps):
        rows = pl.ds(step * mesh_rows, mesh_rows)
        head_rows = silu(acc[rows, :] + dot(gather[4, rows, :], rx[last, 3])).astype(BF16)
        out[rows, :] = dot(head_rows, v_wfinal[...]).astype(BF16)
    for copy in started:
        copy.wait_send()


def body(
    grid_in, dest_block, dest_node, neighbour_mask, mesh_embed, w_in, in_bias, w_grid, w_enc, attn_gain,
    w_query, w_key, w_value, w_out, mlp_gain, w_up, w_down, dec_gain, w_dec, w_head, w_final,
):
    count = lax.axis_size("block")
    grid_rows, channels = grid_in.shape
    mesh_rows, width = mesh_embed.shape
    operands = [
        grid_in,
        dest_block.reshape(1, grid_rows),
        dest_node.reshape(1, grid_rows),
        neighbour_mask.T,
        mesh_embed,
        w_in,
        in_bias.reshape(width // 128, 128),
        w_grid,
        w_enc,
        attn_gain,
        w_query,
        w_key,
        w_value,
        w_out,
        mlp_gain,
        w_up,
        w_down,
        dec_gain.reshape(width // 128, 128),
        w_dec,
        w_head,
        w_final,
    ]
    phases = LAYERS + 1
    scratch = [pltpu.VMEM(operand.shape, operand.dtype) for operand in operands] + [
        pltpu.VMEM((width, width), BF16),
        pltpu.VMEM((width, width), BF16),
        pltpu.VMEM((grid_rows, width), BF16),
        pltpu.VMEM((grid_rows, width), BF16),
        pltpu.VMEM((4, mesh_rows, width), BF16),
        pltpu.VMEM((4, 8, mesh_rows), F32),
        pltpu.VMEM((4, 8, mesh_rows), F32),
        pltpu.VMEM((4, mesh_rows, width), BF16),
        pltpu.VMEM((mesh_rows, width), F32),
        pltpu.VMEM((mesh_rows, width), F32),
        pltpu.VMEM((mesh_rows, width), F32),
        pltpu.VMEM((2, mesh_rows, 128), F32),
        pltpu.VMEM((phases, mesh_rows, width), BF16),
        pltpu.VMEM((phases, 4, mesh_rows, width), BF16),
        pltpu.VMEM((HEADS, mesh_rows, 128), BF16),
        pltpu.VMEM((5, HEADS, mesh_rows, 128), BF16),
        pltpu.VMEM((5, HEADS, mesh_rows, 128), BF16),
        pltpu.VMEM((HEADS, mesh_rows, 128), F32),
        pltpu.VMEM((HEADS, mesh_rows, 128), F32),
        pltpu.VMEM((mesh_rows, width), BF16),
        pltpu.VMEM((5, grid_rows, mesh_rows), BF16),
        pltpu.VMEM((grid_rows, width), F32),
        pltpu.SemaphoreType.DMA((len(operands),)),
        pltpu.SemaphoreType.DMA((12,)),
        pltpu.SemaphoreType.DMA((12,)),
        pltpu.SemaphoreType.DMA((phases, 4, HALVES)),
        pltpu.SemaphoreType.DMA((phases, 4, HALVES)),
    ]
    return pl.pallas_call(
        functools.partial(kernel, count),
        out_shape=pltpu.VMEM((grid_rows, channels), BF16),
        in_specs=[pl.BlockSpec(memory_space=pl.ANY)] * len(operands),
        out_specs=pl.BlockSpec(memory_space=pltpu.VMEM),
        scratch_shapes=scratch,
        compiler_params=pltpu.CompilerParams(
            collective_id=0, has_side_effects=True, vmem_limit_bytes=60 * 1024 * 1024
        ),
        name="step",
    )(*operands)


def solution(mesh):
    rows = P(("member", "block"), None)
    placed = (rows, rows, P(("member", "block")), rows, rows) + (P(),) * 16
    return jax.shard_map(body, mesh=mesh, in_specs=placed, out_specs=rows, check_vma=False)
```
